32 devices in a mesh: img: 4 (over y, x), row: 8 (over z, core).
Axes of the slice: x: 2, y: 2, z: 4, core: 2. Of those that a mesh axis runs over, the one named last changes fastest.
Arguments:
- latent: bfloat16 [128, 128, 512], P(('img', 'row')), parts along dimension 0, may hold values from -8 to 8
- attn_gain: float32 [512], replicated, may hold values from 0.5 to 1.5
- attn_shift: float32 [512], replicated, may hold values from -3 to 3
- w_query: bfloat16 [512, 512], replicated, may hold values from -2 to 2
- w_key: bfloat16 [512, 512], replicated, may hold values from -2 to 2
- w_value: bfloat16 [512, 512], replicated, may hold values from -0.25 to 0.25
- w_out: bfloat16 [512, 512], replicated, may hold values from -0.25 to 0.25
- conv_gain: float32 [512], replicated, may hold values from 0.5 to 1.5
- conv_shift: float32 [512], replicated, may hold values from -3 to 3
- w_conv: bfloat16 [3, 3, 512, 512], replicated, may hold values from -0.09375 to 0.09375
- conv_bias: float32 [512], replicated, may hold values from -3 to 3
Outputs:
- encoded: bfloat16 [128, 128, 512], P(('img', 'row')), parts along dimension 0
The draws below stay inside these ranges and needn't reach their ends.
There are 4 independent parts, one for each index of `img`. The reference program is written for one: setup_inputs(seed, part) draws one part's arguments, and reference() takes and returns one part's arrays. A program takes and returns all parts, laid end to end along the dimension named above; an argument that names none is the same for every part. Nothing has to cross between parts.
All inputs are finite; a program needn't handle non-finite values.
Results may differ from the reference program's by a relative error of at most 0.011.
Values may be sent and summed in bfloat16 or wider, within the bound.
A program may use at most 128 MiB of HBM per device.

```python
import jax
import jax.numpy as jnp
from jax import lax

C = 512
GROUPS = 32
W = 128
H = 32


def shared_gauss(key):
    return jnp.clip(jax.random.normal(jax.random.fold_in(key, 7), (C, C), jnp.float32), -3.0, 3.0)


def draw_latent(key, part):
    noise = jax.random.normal(jax.random.fold_in(key, 3), (H, W, C), jnp.float32)
    rows = (jnp.arange(H, dtype=jnp.float32) + 0.5) / H
    phase = jax.random.uniform(jax.random.fold_in(key, 13), (GROUPS,), jnp.float32, -jnp.pi, jnp.pi)
    amplitude = jax.random.uniform(jax.random.fold_in(key, 17), (C,), jnp.float32, 0.8, 1.6)
    wave = jnp.sin(2.0 * jnp.pi * rows[:, None] + phase[None, :])
    offset = jnp.repeat(wave, C // GROUPS, axis=1) * amplitude[None, :]
    result = noise + offset[:, None, :]
    return jnp.clip(result, -8.0, 8.0).astype(jnp.bfloat16)


def draw_w_query(key, part):
    return (shared_gauss(key) * (4.0 / jnp.sqrt(jnp.float32(C)))).astype(jnp.bfloat16)


def draw_w_key(key, part):
    fresh = jnp.clip(jax.random.normal(jax.random.fold_in(key, 11), (C, C), jnp.float32), -3.0, 3.0)
    result = fresh / jnp.sqrt(jnp.float32(C))
    return result.astype(jnp.bfloat16)


def scatter_about(stream_key, extent, scale, most, kind=jnp.bfloat16):
    return jnp.clip(scale * jax.random.normal(stream_key, extent, jnp.float32), -most, most).astype(kind)


def setup_inputs(seed: int = 0, part: int = 0) -> dict:
    key_list = jax.random.split(jax.random.key(seed), 12)
    part_splits = jax.random.split(jax.random.fold_in(key_list[11], part), 12)
    return {
        "latent": draw_latent(jax.random.fold_in(jax.random.fold_in(key_list[11], part), 71), part),
        "attn_gain": jnp.clip(1.0 + 0.1 * jax.random.normal(key_list[1], (C,), jnp.float32), 0.5, 1.5),
        "attn_shift": scatter_about(key_list[2], (C,), 0.5, 3.0, jnp.float32),
        "w_query": draw_w_query(jax.random.fold_in(key_list[11], 71), part),
        "w_key": draw_w_key(jax.random.fold_in(key_list[11], 71), part),
        "w_value": scatter_about(key_list[5], (C, C), C ** -0.5, 0.25),
        "w_out": scatter_about(key_list[6], (C, C), C ** -0.5, 0.25),
        "conv_gain": jnp.clip(1.0 + 0.1 * jax.random.normal(key_list[7], (C,), jnp.float32), 0.5, 1.5),
        "conv_shift": scatter_about(key_list[8], (C,), 0.5, 3.0, jnp.float32),
        "w_conv": scatter_about(key_list[9], (3, 3, C, C), (9 * C) ** -0.5, 0.09375),
        "conv_bias": scatter_about(key_list[10], (C,), 0.5, 3.0, jnp.float32),
    }


epsilon = 1e-06

def group_norm(field, gain, shift):
    grouped = field.astype(jnp.float32).reshape(field.shape[0], GROUPS, C // GROUPS)
    centre = lax.optimization_barrier(jnp.mean(grouped, axis=(0, 2)))
    offset = grouped - centre[None, :, None]
    spread = lax.optimization_barrier(jnp.mean(offset * offset, axis=(0, 2)))
    normed = offset * lax.rsqrt(spread + epsilon)[None, :, None]
    return normed.reshape(field.shape) * gain + shift

def reference(latent, attn_gain, attn_shift, w_query, w_key, w_value, w_out, conv_gain, conv_shift, w_conv, conv_bias):
    positions = latent.reshape(H * W, C)
    normed = group_norm(positions, attn_gain, attn_shift).astype(jnp.bfloat16)
    queries = jnp.dot(normed, w_query, preferred_element_type=jnp.float32).astype(jnp.bfloat16)
    key_rows = jnp.dot(normed, w_key, preferred_element_type=jnp.float32).astype(jnp.bfloat16)
    values = jnp.dot(normed, w_value, preferred_element_type=jnp.float32).astype(jnp.bfloat16)
    scaling = 1.0 / jnp.sqrt(jnp.float32(C))
    scores = jnp.einsum('qc,kc->qk', queries.astype(jnp.float32), key_rows.astype(jnp.float32)) * scaling
    rowmax = lax.optimization_barrier(jnp.max(scores, axis=1))
    expo = jnp.exp(scores - rowmax[:, None])
    denominator = lax.optimization_barrier(jnp.sum(expo, axis=1))
    probs = expo.astype(jnp.bfloat16)
    attended = (jnp.dot(probs, values, preferred_element_type=jnp.float32) / denominator[:, None]).astype(jnp.bfloat16)
    hidden = (positions.astype(jnp.float32) + jnp.dot(attended, w_out, preferred_element_type=jnp.float32)).astype(jnp.bfloat16)
    activated = jax.nn.silu(group_norm(hidden, conv_gain, conv_shift)).astype(jnp.bfloat16).reshape(H, W, C)
    padded = jnp.pad(activated, ((1, 1), (1, 1), (0, 0)))
    convolved = jnp.zeros((H * W, C), jnp.float32)
    for row_tap in range(3):
        for col_tap in range(3):
            window = padded[row_tap:row_tap + H, col_tap:col_tap + W].reshape(H * W, C)
            convolved = convolved + jnp.dot(window, w_conv[row_tap, col_tap], preferred_element_type=jnp.float32)
    encoded = hidden.astype(jnp.float32) + (convolved + conv_bias)
    return encoded.astype(jnp.bfloat16).reshape(H, W, C)
```

```python
import functools
import math

import jax
import jax.numpy as jnp
from jax import lax
from jax.experimental import pallas as pl
from jax.experimental.pallas import tpu as pltpu
from jax.sharding import PartitionSpec as P

GROUPS = 32
EPS = 1e-06
CHUNK = 128
BAND = 256
MESH = pl.DeviceIdType.MESH
LOG2E = math.log2(math.e)
NT = (((1,), (1,)), ((), ()))


def spread_groups(row, ones):
    high = row.astype(jnp.bfloat16).astype(jnp.float32)
    rest = row - high
    mid = rest.astype(jnp.bfloat16).astype(jnp.float32)
    low = rest - mid
    index = lax.broadcasted_iota(jnp.int32, (16, row.shape[1]), 0)
    parts = jnp.where(index == 0, high, jnp.where(index == 1, mid, jnp.where(index == 2, low, 0.0)))
    sums = jnp.dot(parts.astype(jnp.bfloat16), ones, preferred_element_type=jnp.float32)
    return jnp.sum(sums, axis=0, keepdims=True)


def kernel(
    n, wide,
    latent, w_query, w_key, w_value, w_out, w_conv,
    attn_gain, attn_shift, conv_gain, conv_shift, conv_bias,
    out,
    kv, wq, wk, wv, wo, wc, ones, moments, queries, bias, maxima, total, acc, hidden, halo, stacked,
    load_sem, weight_sem, send_sem, recv_sem, stat_send, stat_recv, halo_send, halo_recv,
):
    chunks, cores, chunk, channels = kv.shape[1:]
    rows = chunks * chunk
    deep = n // 2
    lines = rows // wide
    size = channels // GROUPS
    img = lax.axis_index("img")
    r = lax.axis_index("row")
    z = r // 2
    c = r % 2
    partner = r + 1 - 2 * c

    loads = [
        pltpu.make_async_copy(latent.at[k], kv.at[z, k, c], load_sem.at[k]) for k in range(chunks)
    ]
    for load in loads:
        load.start()
    weights = [
        pltpu.make_async_copy(source, target, weight_sem.at[i])
        for i, (source, target) in enumerate([(w_query, wq), (w_key, wk), (w_value, wv), (w_out, wo)])
    ]
    weights += [
        pltpu.make_async_copy(
            w_conv.at[dy, dx],
            wc.at[dx, pl.ds(dy * channels, channels)],
            weight_sem.at[4 + dy * 3 + dx],
        )
        for dy in range(3)
        for dx in range(3)
    ]

    barrier = pltpu.get_barrier_semaphore()

    @pl.loop(1, n)
    def _(j):
        pl.semaphore_signal(
            barrier, inc=1, device_id=(img, lax.rem(r + j, n)), device_id_type=MESH
        )

    def piece(way, zb, k):
        target = (r + 2, r - 2, partner)[way]
        return pltpu.make_async_remote_copy(
            src_ref=kv.at[zb, k, c],
            dst_ref=kv.at[zb, k, c],
            send_sem=send_sem.at[way, zb, k],
            recv_sem=recv_sem.at[zb, k, c],
            device_id=(img, target),
            device_id_type=MESH,
        )

    def arrival(zb, k, core):
        return pltpu.make_async_remote_copy(
            src_ref=kv.at[zb, k, core],
            dst_ref=kv.at[zb, k, core],
            send_sem=send_sem.at[0, 0, 0],
            recv_sem=recv_sem.at[zb, k, core],
            device_id=(img, partner),
            device_id_type=MESH,
        )

    def stat_copy(which, j):
        return pltpu.make_async_remote_copy(
            src_ref=moments.at[which, r],
            dst_ref=moments.at[which, r],
            send_sem=stat_send.at[which, j],
            recv_sem=stat_recv.at[which, r],
            device_id=(img, lax.rem(r + j, n)),
            device_id_type=MESH,
        )

    def stat_arrival(which, b):
        return pltpu.make_async_remote_copy(
            src_ref=moments.at[which, b],
            dst_ref=moments.at[which, b],
            send_sem=stat_send.at[which, 0],
            recv_sem=stat_recv.at[which, b],
            device_id=(img, partner),
            device_id_type=MESH,
        )

    def own_rows():
        return kv[z, :, c].reshape(rows, channels)

    def send_own(k):
        @pl.when(z < deep - 1)
        def _():
            piece(0, z, k).start()

        @pl.when(z > 0)
        def _():
            piece(1, z, k).start()

        piece(2, z, k).start()

    def share_moments(which, field):
        mean = jnp.sum(field, axis=0, keepdims=True) * (1.0 / rows)
        offset = field - mean
        square = jnp.sum(offset * offset, axis=0, keepdims=True)
        moments[which, r, 0:1, :] = mean
        moments[which, r, 1:2, :] = square

        @pl.loop(1, n)
        def _(j):
            stat_copy(which, j).start()

    def gather_moments(which):
        @pl.loop(1, n)
        def _(j):
            stat_arrival(which, lax.rem(r + j, n)).wait_recv()

        @pl.loop(1, n)
        def _(j):
            stat_copy(which, j).wait_send()

        every = moments[which]
        means = every[:, 0, :]
        squares = every[:, 1, :]
        centre = spread_groups(jnp.sum(means, axis=0, keepdims=True), ones[...]) * (
            1.0 / (n * size)
        )
        away = means - centre
        whole = jnp.sum(squares + rows * (away * away), axis=0, keepdims=True)
        variance = spread_groups(whole, ones[...]) * (1.0 / (n * size * rows))
        return centre, lax.rsqrt(variance + EPS)

    with jax.named_scope("load"):
        for load in loads:
            load.wait()
    for weight in weights:
        weight.start()
    with jax.named_scope("barrier"):
        pl.semaphore_wait(barrier, n - 1)
    with jax.named_scope("share0"):
        send_own(0)
        share_moments(0, own_rows().astype(jnp.float32))
        for k in range(1, chunks):
            send_own(k)

    left_group = lax.broadcasted_iota(jnp.int32, (channels, channels), 0) // size
    right_group = lax.broadcasted_iota(jnp.int32, (channels, channels), 1) // size
    ones[...] = jnp.where(left_group == right_group, 1.0, 0.0).astype(jnp.bfloat16)
    maxima[...] = jnp.full_like(maxima, -1e30)
    total[...] = jnp.zeros_like(total)
    acc[...] = jnp.zeros_like(acc)

    for weight in weights[:4]:
        weight.wait()
    with jax.named_scope("fold"):
        wv[...] = jnp.dot(wv[...], wo[...], preferred_element_type=jnp.float32).astype(jnp.bfloat16)
    with jax.named_scope("stat0"):
        centre, scale = gather_moments(0)
    gain = scale * attn_gain[...]
    positions = own_rows().astype(jnp.float32)
    normed = ((positions - centre) * gain + attn_shift[...]).astype(jnp.bfloat16)
    query = jnp.dot(normed, wq[...], preferred_element_type=jnp.float32).astype(jnp.bfloat16)
    folded = lax.dot_general(query, wk[...], NT, preferred_element_type=jnp.float32) * (
        LOG2E / math.sqrt(channels)
    )
    queries[...] = (folded * gain).astype(jnp.bfloat16)
    constant = jnp.sum(folded * (attn_shift[...] - centre * gain), axis=1, keepdims=True)
    bias[...] = jnp.broadcast_to(constant, bias.shape)

    def attend(zb, k):
        block = kv[zb, k].reshape(cores * chunk, channels)
        for start in range(0, rows, BAND):
            band = slice(start, start + BAND)
            scores = lax.dot_general(
                queries[band], block, NT, preferred_element_type=jnp.float32
            )
            scores = scores + jnp.tile(bias[band], (1, cores * chunk // 128))
            newest = jnp.maximum(maxima[band], jnp.max(scores, axis=1, keepdims=True))
            fade = jnp.exp2(maxima[band] - newest)
            maxima[band] = newest
            expo = jnp.exp2(scores - jnp.tile(newest, (1, cores * chunk // 128)))
            summed = total[band] * fade
            for j in range(cores * chunk // 128):
                summed = summed + expo[:, j * 128 : (j + 1) * 128]
            total[band] = summed
            product = jnp.dot(
                expo.astype(jnp.bfloat16), block, preferred_element_type=jnp.float32
            )
            acc[band] = acc[band] * jnp.tile(fade, (1, channels // 128)) + product

    def relay(t):
        d = t // chunks
        k = t % chunks
        for way, zb in ((0, z - d), (1, z + d)):
            inside = jnp.logical_and(d > 0, jnp.logical_and(zb >= 0, zb < deep))

            @pl.when(inside)
            def _(way=way, zb=zb):
                arrival(zb, k, c).wait_recv()

                @pl.when((z < deep - 1) if way == 0 else (z > 0))
                def _():
                    piece(way, zb, k).start()

                piece(2, zb, k).start()

    ahead = jnp.where(jnp.logical_and(z > 0, z < deep - 1), chunks, 0)

    @pl.loop(0, deep * chunks)
    def _(t):
        with jax.named_scope("relay"):
            relay(t + ahead)
        d = t // chunks
        k = t % chunks

        @pl.loop(0, 2)
        def _(side):
            zb = z + d * (2 * side - 1)
            inside = jnp.logical_and(zb >= 0, zb < deep)

            @pl.when(jnp.logical_and(inside, jnp.logical_or(side == 0, d > 0)))
            def _():
                with jax.named_scope("wait"):
                    arrival(zb, k, 1 - c).wait_recv()
                with jax.named_scope("attend"):
                    attend(zb, k)

    with jax.named_scope("post"):
        denominator = jnp.sum(total[...], axis=1, keepdims=True)
        average = (acc[...] / denominator - centre) * gain + attn_shift[...]
        field = (
            own_rows().astype(jnp.float32)
            + jnp.dot(average.astype(jnp.bfloat16), wv[...], preferred_element_type=jnp.float32)
        ).astype(jnp.bfloat16)
        hidden[...] = field
        share_moments(1, field.astype(jnp.float32))

    up = pltpu.make_async_remote_copy(
        src_ref=hidden.at[pl.ds(0, wide)],
        dst_ref=halo.at[1],
        send_sem=halo_send.at[1],
        recv_sem=halo_recv.at[1],
        device_id=(img, r - 1),
        device_id_type=MESH,
    )
    down = pltpu.make_async_remote_copy(
        src_ref=hidden.at[pl.ds(rows - wide, wide)],
        dst_ref=halo.at[0],
        send_sem=halo_send.at[0],
        recv_sem=halo_recv.at[0],
        device_id=(img, r + 1),
        device_id_type=MESH,
    )

    @pl.when(r > 0)
    def _():
        up.start()

    @pl.when(r < n - 1)
    def _():
        down.start()

    @pl.loop(0, deep * chunks)
    def _(t):
        zb = t // chunks
        k = t % chunks

        @pl.when(jnp.logical_and(z < deep - 1, zb <= z))
        def _():
            piece(0, zb, k).wait_send()

        @pl.when(jnp.logical_and(z > 0, zb >= z))
        def _():
            piece(1, zb, k).wait_send()

        piece(2, zb, k).wait_send()

    for weight in weights[4:]:
        weight.wait()
    with jax.named_scope("stat1"):
        centre, scale = gather_moments(1)
    gain = scale * conv_gain[...]

    def activate(values):
        v = (values.astype(jnp.float32) - centre) * gain + conv_shift[...]
        return (v / (1.0 + jnp.exp(-v))).astype(jnp.bfloat16)

    def place(line, values):
        for dy in range(3):
            y = line + 1 - dy
            if 0 <= y < lines:
                stacked[y * wide : (y + 1) * wide, dy * channels : (dy + 1) * channels] = values

    with jax.named_scope("act"):
      for line in range(lines):
        place(line, activate(hidden[line * wide : (line + 1) * wide]))

    @pl.when(r > 0)
    def _():
        up.wait_send()
        down.wait_recv()
        place(-1, activate(halo[0]))

    @pl.when(r == 0)
    def _():
        place(-1, jnp.zeros((wide, channels), jnp.bfloat16))

    @pl.when(r < n - 1)
    def _():
        down.wait_send()
        up.wait_recv()
        place(lines, activate(halo[1]))

    @pl.when(r == n - 1)
    def _():
        place(lines, jnp.zeros((wide, channels), jnp.bfloat16))

    half = 256
    column = lax.broadcasted_iota(jnp.int32, (rows, half), 0) % wide
    with jax.named_scope("conv"):
      for start in range(0, channels, half):
        cut = slice(start, start + half)

        def taps(dx):
            return jnp.dot(stacked[...], wc[dx, :, cut], preferred_element_type=jnp.float32)

        convolved = taps(1)
        convolved = convolved + jnp.where(column > 0, pltpu.roll(taps(0), 1, 0), 0.0)
        convolved = convolved + jnp.where(
            column < wide - 1, pltpu.roll(taps(2), rows - 1, 0), 0.0
        )
        encoded = hidden[:, cut].astype(jnp.float32) + (convolved + conv_bias[:, cut])
        out[:, cut] = encoded.astype(jnp.bfloat16)


def local(n, latent, attn_gain, attn_shift, w_query, w_key, w_value, w_out,
          conv_gain, conv_shift, w_conv, conv_bias):
    height, wide, channels = latent.shape
    rows = height * wide
    chunks = rows // CHUNK
    anywhere = pl.BlockSpec(memory_space=pl.ANY)
    vmem = pl.BlockSpec(memory_space=pltpu.VMEM)
    bf16, f32 = jnp.bfloat16, jnp.float32
    square = pltpu.VMEM((channels, channels), bf16)
    dma = pltpu.SemaphoreType.DMA
    encoded = pl.pallas_call(
        functools.partial(kernel, n, wide),
        out_shape=pltpu.VMEM((rows, channels), bf16),
        in_specs=[anywhere] * 6 + [vmem] * 5,
        out_specs=vmem,
        scratch_shapes=[
            pltpu.VMEM((n // 2, chunks, 2, CHUNK, channels), bf16),
            square, square, square, square,
            pltpu.VMEM((3, 3 * channels, channels), bf16),
            square,
            pltpu.VMEM((2, n, 2, channels), f32),
            pltpu.VMEM((rows, channels), bf16),
            pltpu.VMEM((rows, 128), f32),
            pltpu.VMEM((rows, 128), f32),
            pltpu.VMEM((rows, 128), f32),
            pltpu.VMEM((rows, channels), f32),
            pltpu.VMEM((rows, channels), bf16),
            pltpu.VMEM((2, wide, channels), bf16),
            pltpu.VMEM((rows, 3 * channels), bf16),
            dma((chunks,)),
            dma((13,)),
            dma((3, n // 2, chunks)),
            dma((n // 2, chunks, 2)),
            dma((2, n)),
            dma((2, n)),
            dma((2,)),
            dma((2,)),
        ],
        compiler_params=pltpu.CompilerParams(
            collective_id=0, has_side_effects=True, vmem_limit_bytes=56 * 1024 * 1024
        ),
    )(
        latent.reshape(chunks, CHUNK, channels), w_query, w_key, w_value, w_out, w_conv,
        *(v.reshape(1, channels) for v in (attn_gain, attn_shift, conv_gain, conv_shift, conv_bias)),
    )
    return encoded.reshape(height, wide, channels)


def solution(mesh):
    in_specs = (P(("img", "row"), None, None), P(), P(), P(), P(), P(), P(), P(), P(), P(), P())
    out_specs = P(("img", "row"), None, None)
    body = functools.partial(local, mesh.shape["row"])
    return jax.shard_map(body, mesh=mesh, in_specs=in_specs, out_specs=out_specs, check_vma=False)
```

```python
import functools
import math

import jax
import jax.numpy as jnp
from jax import lax
from jax.experimental import pallas as pl
from jax.experimental.pallas import tpu as pltpu
from jax.sharding import PartitionSpec as P

GROUPS = 32
EPS = 1e-06
CHUNK = 128
BAND = 512
MESH = pl.DeviceIdType.MESH
LOG2E = math.log2(math.e)
NT = (((1,), (1,)), ((), ()))


def spread_groups(row, ones):
    high = row.astype(jnp.bfloat16).astype(jnp.float32)
    rest = row - high
    mid = rest.astype(jnp.bfloat16).astype(jnp.float32)
    low = rest - mid
    index = lax.broadcasted_iota(jnp.int32, (16, row.shape[1]), 0)
    parts = jnp.where(index == 0, high, jnp.where(index == 1, mid, jnp.where(index == 2, low, 0.0)))
    sums = jnp.dot(parts.astype(jnp.bfloat16), ones, preferred_element_type=jnp.float32)
    return jnp.sum(sums, axis=0, keepdims=True)


def kernel(
    n, wide,
    latent, w_query, w_key, w_value, w_out, w_conv,
    gain_in, shift_in, conv_gain_in, conv_shift_in, bias_in,
    out,
    vector, kv, square, wc, ones, moments, queries, bias, maxima, total, acc, hidden, halo, stacked,
    load_sem, weight_sem, send_sem, recv_sem, stat_send, stat_recv, halo_send, halo_recv,
    vector_sem, present,
):
    chunks, cores, chunk, channels = kv.shape[1:]
    rows = chunks * chunk
    deep = n // 2
    lines = rows // wide
    size = channels // GROUPS
    img = lax.axis_index("img")
    r = lax.axis_index("row")
    z = r // 2
    c = r % 2
    partner = r + 1 - 2 * c

    load = pltpu.make_async_copy(latent, kv.at[z, :, c], load_sem)
    load.start()

    barrier = pltpu.get_barrier_semaphore()

    def neighbours(act):
        @pl.when(z < deep - 1)
        def _():
            act(r + 2)

        @pl.when(z > 0)
        def _():
            act(r - 2)

        act(partner)

    def signal(semaphore, target):
        pl.semaphore_signal(semaphore, inc=1, device_id=(img, target), device_id_type=MESH)

    neighbours(functools.partial(signal, barrier))
    vectors = [
        pltpu.make_async_copy(source, vector.at[i], vector_sem)
        for i, source in enumerate((gain_in, shift_in, conv_gain_in, conv_shift_in, bias_in))
    ]
    attn_gain, attn_shift, conv_gain, conv_shift, conv_bias = (vector.at[i] for i in range(5))
    wq, wk, wv, wo = (square.at[i] for i in range(4))
    weights = [
        pltpu.make_async_copy(source, square.at[i], weight_sem.at[0])
        for i, source in enumerate((w_query, w_key, w_value, w_out))
    ]
    taps_in = pltpu.make_async_copy(w_conv, wc, weight_sem.at[1])

    def piece(way, zb, k):
        target = (r + 2, r - 2, partner)[way]
        return pltpu.make_async_remote_copy(
            src_ref=kv.at[zb, k, c],
            dst_ref=kv.at[zb, k, c],
            send_sem=send_sem.at[way],
            recv_sem=recv_sem.at[zb, k, c],
            device_id=(img, target),
            device_id_type=MESH,
        )

    def arrival(zb, k, core):
        return pltpu.make_async_remote_copy(
            src_ref=kv.at[zb, k, core],
            dst_ref=kv.at[zb, k, core],
            send_sem=send_sem.at[0],
            recv_sem=recv_sem.at[zb, k, core],
            device_id=(img, partner),
            device_id_type=MESH,
        )

    def stat_copy(which, j):
        return pltpu.make_async_remote_copy(
            src_ref=moments.at[which, r],
            dst_ref=moments.at[which, r],
            send_sem=stat_send.at[which],
            recv_sem=stat_recv.at[which],
            device_id=(img, lax.rem(r + j, n)),
            device_id_type=MESH,
        )

    def stat_all(which):
        return pltpu.make_async_remote_copy(
            src_ref=moments.at[which, pl.ds(0, n - 1)],
            dst_ref=moments.at[which, pl.ds(0, n - 1)],
            send_sem=stat_send.at[which],
            recv_sem=stat_recv.at[which],
            device_id=(img, partner),
            device_id_type=MESH,
        )

    def own_rows():
        return kv[z, :, c].reshape(rows, channels)

    def send_own(k):
        @pl.when(z < deep - 1)
        def _():
            piece(0, z, k).start()

        @pl.when(z > 0)
        def _():
            piece(1, z, k).start()

        piece(2, z, k).start()

    def find_moments(which, field):
        mean = jnp.sum(field, axis=0, keepdims=True) * (1.0 / rows)
        offset = field - mean
        square = jnp.sum(offset * offset, axis=0, keepdims=True)
        moments[which, r, 0:1, :] = mean
        moments[which, r, 1:2, :] = square

    def share_moments(which):
        @pl.loop(1, n)
        def _(j):
            stat_copy(which, j).start()

    def gather_moments(which):
        stat_all(which).wait_recv()
        stat_all(which).wait_send()
        every = moments[which]
        means = every[:, 0, :]
        squares = every[:, 1, :]
        centre = spread_groups(jnp.sum(means, axis=0, keepdims=True), ones[...]) * (
            1.0 / (n * size)
        )
        away = means - centre
        whole = jnp.sum(squares + rows * (away * away), axis=0, keepdims=True)
        variance = spread_groups(whole, ones[...]) * (1.0 / (n * size * rows))
        return centre, lax.rsqrt(variance + EPS)

    with jax.named_scope("load"):
        load.wait()
    with jax.named_scope("barrier"):
        pl.semaphore_wait(barrier, 1 + (z > 0).astype(jnp.int32) + (z < deep - 1).astype(jnp.int32))

    early = chunks // 2

    @pl.when(c == 0)
    def _():
        for k in range(early):
            send_own(k)

    for copy in vectors + weights + [taps_in]:
        copy.start()
    with jax.named_scope("share0"):
        find_moments(0, own_rows().astype(jnp.float32))

    @pl.when(c == 1)
    def _():
        for k in range(early):
            send_own(k)

    def chain(way):
        first, last = (z == 0, z == deep - 1) if way == 0 else (z == deep - 1, z == 0)

        @pl.when(jnp.logical_not(first))
        def _():
            pl.semaphore_wait(present.at[way], 1)

        @pl.when(jnp.logical_not(last))
        def _():
            signal(present.at[way], r + 2 - 4 * way)

    with jax.named_scope("present"):
        @pl.when(z < deep // 2)
        def _():
            chain(0)
            chain(1)

        @pl.when(z >= deep // 2)
        def _():
            chain(1)
            chain(0)

        signal(present.at[2], partner)
        pl.semaphore_wait(present.at[2], 1)
    share_moments(0)
    for k in range(early, chunks):
        send_own(k)

    left_group = lax.broadcasted_iota(jnp.int32, (channels, channels), 0) // size
    right_group = lax.broadcasted_iota(jnp.int32, (channels, channels), 1) // size
    ones[...] = jnp.where(left_group == right_group, 1.0, 0.0).astype(jnp.bfloat16)
    maxima[...] = jnp.full_like(maxima, -1e30)
    total[...] = jnp.zeros_like(total)
    acc[...] = jnp.zeros_like(acc)

    pltpu.make_async_copy(vector, vector, vector_sem).wait()
    pltpu.make_async_copy(square, square, weight_sem.at[0]).wait()
    with jax.named_scope("fold"):
        wv[...] = jnp.dot(wv[...], wo[...], preferred_element_type=jnp.float32).astype(jnp.bfloat16)
    with jax.named_scope("stat0"):
        centre, scale = gather_moments(0)
    gain = scale * attn_gain[...]
    positions = own_rows().astype(jnp.float32)
    normed = ((positions - centre) * gain + attn_shift[...]).astype(jnp.bfloat16)
    query = jnp.dot(normed, wq[...], preferred_element_type=jnp.float32).astype(jnp.bfloat16)
    folded = lax.dot_general(query, wk[...], NT, preferred_element_type=jnp.float32) * (
        LOG2E / math.sqrt(channels)
    )
    queries[...] = (folded * gain).astype(jnp.bfloat16)
    constant = jnp.sum(folded * (attn_shift[...] - centre * gain), axis=1, keepdims=True)
    bias[...] = jnp.broadcast_to(constant, bias.shape)

    def attend(zb, k):
        block = kv[zb, k].reshape(cores * chunk, channels)
        for start in range(0, rows, BAND):
            band = slice(start, start + BAND)
            scores = lax.dot_general(
                queries[band], block, NT, preferred_element_type=jnp.float32
            )
            scores = scores + jnp.tile(bias[band], (1, cores * chunk // 128))
            newest = jnp.maximum(maxima[band], jnp.max(scores, axis=1, keepdims=True))
            fade = jnp.exp2(maxima[band] - newest)
            maxima[band] = newest
            expo = jnp.exp2(scores - jnp.tile(newest, (1, cores * chunk // 128)))
            summed = total[band] * fade
            for j in range(cores * chunk // 128):
                summed = summed + expo[:, j * 128 : (j + 1) * 128]
            total[band] = summed
            product = jnp.dot(
                expo.astype(jnp.bfloat16), block, preferred_element_type=jnp.float32
            )
            acc[band] = acc[band] * jnp.tile(fade, (1, channels // 128)) + product

    def relay(t):
        d = t // chunks
        k = t % chunks
        for way, zb in ((0, z - d), (1, z + d)):
            inside = jnp.logical_and(d > 0, jnp.logical_and(zb >= 0, zb < deep))

            @pl.when(inside)
            def _(way=way, zb=zb):
                arrival(zb, k, c).wait_recv()

                @pl.when((z < deep - 1) if way == 0 else (z > 0))
                def _():
                    piece(way, zb, k).start()

                piece(2, zb, k).start()

    ahead = jnp.where(jnp.logical_and(z > 0, z < deep - 1), chunks, 0)

    @pl.loop(0, deep * chunks)
    def _(t):
        with jax.named_scope("relay"):
            relay(t + ahead)
        d = t // chunks
        k = t % chunks

        @pl.loop(0, 2)
        def _(side):
            zb = z + d * (2 * side - 1)
            inside = jnp.logical_and(zb >= 0, zb < deep)

            @pl.when(jnp.logical_and(inside, jnp.logical_or(side == 0, d > 0)))
            def _():
                with jax.named_scope("wait"):
                    arrival(zb, k, 1 - c).wait_recv()
                with jax.named_scope("attend"):
                    attend(zb, k)

    with jax.named_scope("post"):
        denominator = jnp.sum(total[...], axis=1, keepdims=True)
        average = (acc[...] / denominator - centre) * gain + attn_shift[...]
        field = (
            own_rows().astype(jnp.float32)
            + jnp.dot(average.astype(jnp.bfloat16), wv[...], preferred_element_type=jnp.float32)
        ).astype(jnp.bfloat16)
        hidden[...] = field
        find_moments(1, field.astype(jnp.float32))
        share_moments(1)

    up = pltpu.make_async_remote_copy(
        src_ref=hidden.at[pl.ds(0, wide)],
        dst_ref=halo.at[1],
        send_sem=halo_send.at[1],
        recv_sem=halo_recv.at[1],
        device_id=(img, r - 1),
        device_id_type=MESH,
    )
    down = pltpu.make_async_remote_copy(
        src_ref=hidden.at[pl.ds(rows - wide, wide)],
        dst_ref=halo.at[0],
        send_sem=halo_send.at[0],
        recv_sem=halo_recv.at[0],
        device_id=(img, r + 1),
        device_id_type=MESH,
    )

    @pl.when(r > 0)
    def _():
        up.start()

    @pl.when(r < n - 1)
    def _():
        down.start()

    def sent(way, first, last):
        part = kv.at[pl.ds(first, last - first), :, c]
        pltpu.make_async_remote_copy(
            src_ref=part,
            dst_ref=part,
            send_sem=send_sem.at[way],
            recv_sem=recv_sem.at[0, 0, 0],
            device_id=(img, partner),
            device_id_type=MESH,
        ).wait_send()

    for here in range(deep):
        @pl.when(z == here)
        def _(here=here):
            if here < deep - 1:
                sent(0, 0, here + 1)
            if here > 0:
                sent(1, here, deep)

    sent(2, 0, deep)

    taps_in.wait()
    with jax.named_scope("stat1"):
        centre, scale = gather_moments(1)
    gain = scale * conv_gain[...]

    def activate(values):
        v = (values.astype(jnp.float32) - centre) * gain + conv_shift[...]
        return (v / (1.0 + jnp.exp(-v))).astype(jnp.bfloat16)

    def place(line, values):
        for dy in range(3):
            y = line + 1 - dy
            if 0 <= y < lines:
                stacked[y * wide : (y + 1) * wide, dy * channels : (dy + 1) * channels] = values

    with jax.named_scope("act"):
      for line in range(lines):
        place(line, activate(hidden[line * wide : (line + 1) * wide]))

    @pl.when(r > 0)
    def _():
        up.wait_send()
        down.wait_recv()
        place(-1, activate(halo[0]))

    @pl.when(r == 0)
    def _():
        place(-1, jnp.zeros((wide, channels), jnp.bfloat16))

    @pl.when(r < n - 1)
    def _():
        down.wait_send()
        up.wait_recv()
        place(lines, activate(halo[1]))

    @pl.when(r == n - 1)
    def _():
        place(lines, jnp.zeros((wide, channels), jnp.bfloat16))

    half = 256
    column = lax.broadcasted_iota(jnp.int32, (rows, half), 0) % wide
    with jax.named_scope("conv"):
      for start in range(0, channels, half):
        cut = slice(start, start + half)

        def taps(dx):
            return jnp.dot(stacked[...], wc[:, dx, :, cut].reshape(3 * channels, half), preferred_element_type=jnp.float32)

        convolved = taps(1)
        convolved = convolved + jnp.where(column > 0, pltpu.roll(taps(0), 1, 0), 0.0)
        convolved = convolved + jnp.where(
            column < wide - 1, pltpu.roll(taps(2), rows - 1, 0), 0.0
        )
        encoded = hidden[:, cut].astype(jnp.float32) + (convolved + conv_bias[:, cut])
        out[:, cut] = encoded.astype(jnp.bfloat16)


def local(n, latent, attn_gain, attn_shift, w_query, w_key, w_value, w_out,
          conv_gain, conv_shift, w_conv, conv_bias):
    height, wide, channels = latent.shape
    rows = height * wide
    chunks = rows // CHUNK
    anywhere = pl.BlockSpec(memory_space=pl.ANY)
    bf16, f32 = jnp.bfloat16, jnp.float32
    dma = pltpu.SemaphoreType.DMA
    encoded = pl.pallas_call(
        functools.partial(kernel, n, wide),
        out_shape=pltpu.VMEM((rows, channels), bf16),
        in_specs=[anywhere] * 11,
        out_specs=pl.BlockSpec(memory_space=pltpu.VMEM),
        scratch_shapes=[
            pltpu.VMEM((5, 1, channels), f32),
            pltpu.VMEM((n // 2, chunks, 2, CHUNK, channels), bf16),
            pltpu.VMEM((4, channels, channels), bf16),
            pltpu.VMEM((3, 3, channels, channels), bf16),
            pltpu.VMEM((channels, channels), bf16),
            pltpu.VMEM((2, n, 2, channels), f32),
            pltpu.VMEM((rows, channels), bf16),
            pltpu.VMEM((rows, 128), f32),
            pltpu.VMEM((rows, 128), f32),
            pltpu.VMEM((rows, 128), f32),
            pltpu.VMEM((rows, channels), f32),
            pltpu.VMEM((rows, channels), bf16),
            pltpu.VMEM((2, wide, channels), bf16),
            pltpu.VMEM((rows, 3 * channels), bf16),
            dma,
            dma((2,)),
            dma((3,)),
            dma((n // 2, chunks, 2)),
            dma((2,)),
            dma((2,)),
            dma((2,)),
            dma((2,)),
            dma,
            pltpu.SemaphoreType.REGULAR((3,)),
        ],
        compiler_params=pltpu.CompilerParams(
            collective_id=0, has_side_effects=True, vmem_limit_bytes=56 * 1024 * 1024
        ),
    )(
        latent.reshape(chunks, CHUNK, channels), w_query, w_key, w_value, w_out, w_conv,
        *(v.reshape(1, channels) for v in (attn_gain, attn_shift, conv_gain, conv_shift, conv_bias)),
    )
    return encoded.reshape(height, wide, channels)


def solution(mesh):
    in_specs = (P(("img", "row"), None, None), P(), P(), P(), P(), P(), P(), P(), P(), P(), P())
    out_specs = P(("img", "row"), None, None)
    body = functools.partial(local, mesh.shape["row"])
    return jax.shard_map(body, mesh=mesh, in_specs=in_specs, out_specs=out_specs, check_vma=False)
```

```python
import functools
import math

import jax
import jax.numpy as jnp
from jax import lax
from jax.experimental import pallas as pl
from jax.experimental.pallas import tpu as pltpu
from jax.sharding import PartitionSpec as P

GROUPS = 32
EPS = 1e-06
CHUNK = 128
UNIT = 2
GROUP = 4
DETOUR = 2
PIECE = 64
MESH = pl.DeviceIdType.MESH
LOG2E = math.log2(math.e)
NT = (((1,), (1,)), ((), ()))


def spread_groups(row, ones):
    high = row.astype(jnp.bfloat16).astype(jnp.float32)
    rest = row - high
    mid = rest.astype(jnp.bfloat16).astype(jnp.float32)
    low = rest - mid
    index = lax.broadcasted_iota(jnp.int32, (16, row.shape[1]), 0)
    parts = jnp.where(index == 0, high, jnp.where(index == 1, mid, jnp.where(index == 2, low, 0.0)))
    sums = jnp.dot(parts.astype(jnp.bfloat16), ones, preferred_element_type=jnp.float32)
    return jnp.sum(sums, axis=0, keepdims=True)


def kernel(
    n, relief, wide,
    latent, w_query, w_key, w_value, w_out, w_conv,
    gain_in, shift_in, conv_gain_in, conv_shift_in, bias_in,
    out,
    vector, kv, square, wc, ones, moments, queries, bias, maxima, total, acc, hidden, halo, stacked,
    load_sem, weight_sem, send_sem, recv_sem, stat_send, stat_recv, halo_send, halo_recv,
    vector_sem, present,
    detour, detour_recv, outgoing, answer, answer_recv, relayed, relayed_recv,
):
    chunks, cores, chunk, channels = kv.shape[1:]
    rows = chunks * chunk
    deep = n // 2
    lines = rows // wide
    size = channels // GROUPS
    img = lax.axis_index("img")
    r = lax.axis_index("row")
    z = r // 2
    c = r % 2
    partner = r + 1 - 2 * c
    both = jnp.logical_and
    no = jnp.logical_not
    units = chunks // UNIT
    early = chunks // 2

    member = img % GROUP
    chief = img - member + GROUP - 1
    is_chief = both(relief, member == GROUP - 1)
    is_member = both(relief, member < GROUP - 1)
    lower, upper = z == 1, z == deep - 2
    inner = jnp.logical_or(lower, upper)
    outer = jnp.logical_or(z == 0, z == deep - 1)
    double = both(is_chief, inner)
    idle = both(is_chief, outer)
    helper = both(is_member, inner)
    late = both(is_member, outer)
    outward = 1 - 2 * lower.astype(jnp.int32)
    inward = 1 - 2 * (z > 0).astype(jnp.int32)
    way_out = lower.astype(jnp.int32)
    direct = chunks - DETOUR
    pieces = rows // PIECE
    routes = [
        GROUP - 1 if p < pieces // 2 else GROUP - 2 - p % 2 for p in range(pieces)
    ]
    legs = [p for p in range(pieces) if routes[p] == GROUP - 2]
    slots = len(legs)

    load = pltpu.make_async_copy(latent, kv.at[z, :, c], load_sem)
    load.start()

    barrier = pltpu.get_barrier_semaphore()

    def neighbours(act):
        @pl.when(z < deep - 1)
        def _():
            act(r + 2)

        @pl.when(z > 0)
        def _():
            act(r - 2)

        act(partner)

    def signal(semaphore, target, image=img):
        pl.semaphore_signal(semaphore, inc=1, device_id=(image, target), device_id_type=MESH)

    neighbours(functools.partial(signal, barrier))
    expected = 1 + (z > 0).astype(jnp.int32) + (z < deep - 1).astype(jnp.int32)
    if relief:
        for i in range(GROUP - 1):
            @pl.when(double)
            def _(i=i):
                signal(barrier, r, chief - GROUP + 1 + i)

        expected = expected + helper.astype(jnp.int32)
    vectors = [
        pltpu.make_async_copy(source, vector.at[i], vector_sem)
        for i, source in enumerate((gain_in, shift_in, conv_gain_in, conv_shift_in, bias_in))
    ]
    attn_gain, attn_shift, conv_gain, conv_shift, conv_bias = (vector.at[i] for i in range(5))
    wq, wk, wv, wo = (square.at[i] for i in range(4))
    weights = [
        pltpu.make_async_copy(source, square.at[i], weight_sem.at[0])
        for i, source in enumerate((w_query, w_key, w_value, w_out))
    ]
    taps_in = pltpu.make_async_copy(w_conv, wc, weight_sem.at[1])

    def piece(way, zb, k):
        target = (r + 2, r - 2, partner)[way]
        return pltpu.make_async_remote_copy(
            src_ref=kv.at[zb, k, c],
            dst_ref=kv.at[zb, k, c],
            send_sem=send_sem.at[way],
            recv_sem=recv_sem.at[zb, k, c],
            device_id=(img, target),
            device_id_type=MESH,
        )

    def arrival(zb, k, core):
        return pltpu.make_async_remote_copy(
            src_ref=kv.at[zb, k, core],
            dst_ref=kv.at[zb, k, core],
            send_sem=send_sem.at[0],
            recv_sem=recv_sem.at[zb, k, core],
            device_id=(img, partner),
            device_id_type=MESH,
        )

    def stat_copy(which, j):
        return pltpu.make_async_remote_copy(
            src_ref=moments.at[which, r],
            dst_ref=moments.at[which, r],
            send_sem=stat_send.at[which],
            recv_sem=stat_recv.at[which],
            device_id=(img, lax.rem(r + j, n)),
            device_id_type=MESH,
        )

    def stat_all(which):
        return pltpu.make_async_remote_copy(
            src_ref=moments.at[which, pl.ds(0, n - 1)],
            dst_ref=moments.at[which, pl.ds(0, n - 1)],
            send_sem=stat_send.at[which],
            recv_sem=stat_recv.at[which],
            device_id=(img, partner),
            device_id_type=MESH,
        )

    def own_rows():
        return kv[z, :, c].reshape(rows, channels)

    def hop(source, target, send, recv, image, row):
        return pltpu.make_async_remote_copy(
            src_ref=source,
            dst_ref=target,
            send_sem=send,
            recv_sem=recv,
            device_id=(image, row),
            device_id_type=MESH,
        )

    def detour_in(i, k):
        return hop(
            kv.at[z, k, c], detour.at[i, k - direct], send_sem.at[way_out],
            detour_recv.at[i, k - direct], chief, r,
        )

    def detour_out(i, k):
        return hop(
            detour.at[i, k - direct], kv.at[z, k, c], send_sem.at[way_out],
            recv_sem.at[z, k, c], chief - GROUP + 1 + i, r + 2 * outward,
        )

    def forward_detours(which):
        for i, k in which:
            detour_in(i, k).wait_recv()
            detour_out(i, k).start()

    far = [(i, k) for k in range(direct, chunks) for i in reversed(range(GROUP - 2))]

    def open_way(way, k=0):
        edge, gate = (z < deep - 1, upper) if way == 0 else (z > 0, lower)
        shut = jnp.logical_or(is_chief, both(is_member, k >= direct))
        return both(edge, no(both(gate, shut)))

    def send_own(k):
        for way in range(2):
            @pl.when(open_way(way, k))
            def _(way=way):
                piece(way, z, k).start()

        @pl.when(no(idle))
        def _():
            piece(2, z, k).start()

    def send_detours():
        if relief:
            @pl.when(helper)
            def _():
                for k in range(direct, chunks):
                    detour_in(member, k).start()

    def find_moments(which, field):
        mean = jnp.sum(field, axis=0, keepdims=True) * (1.0 / rows)
        offset = field - mean
        square = jnp.sum(offset * offset, axis=0, keepdims=True)
        moments[which, r, 0:1, :] = mean
        moments[which, r, 1:2, :] = square

    def share_moments(which):
        @pl.loop(1, n)
        def _(j):
            stat_copy(which, j).start()

    def gather_moments(which):
        stat_all(which).wait_recv()
        stat_all(which).wait_send()
        every = moments[which]
        means = every[:, 0, :]
        squares = every[:, 1, :]
        centre = spread_groups(jnp.sum(means, axis=0, keepdims=True), ones[...]) * (
            1.0 / (n * size)
        )
        away = means - centre
        whole = jnp.sum(squares + rows * (away * away), axis=0, keepdims=True)
        variance = spread_groups(whole, ones[...]) * (1.0 / (n * size * rows))
        return centre, lax.rsqrt(variance + EPS)

    with jax.named_scope("load"):
        load.wait()
    with jax.named_scope("barrier"):
        pl.semaphore_wait(barrier, expected)

    @pl.when(c == 0)
    def _():
        for k in range(early):
            send_own(k)
        send_detours()

    for copy in vectors + weights + [taps_in]:
        copy.start()
    with jax.named_scope("share0"):
        find_moments(0, own_rows().astype(jnp.float32))

    @pl.when(c == 1)
    def _():
        for k in range(early):
            send_own(k)
        send_detours()

    def chain(way):
        first, last = (z == 0, z == deep - 1) if way == 0 else (z == deep - 1, z == 0)

        @pl.when(jnp.logical_not(first))
        def _():
            pl.semaphore_wait(present.at[way], 1)

        @pl.when(jnp.logical_not(last))
        def _():
            signal(present.at[way], r + 2 - 4 * way)

    with jax.named_scope("present"):
        @pl.when(z < deep // 2)
        def _():
            chain(0)
            chain(1)

        @pl.when(z >= deep // 2)
        def _():
            chain(1)
            chain(0)

        signal(present.at[2], partner)
        pl.semaphore_wait(present.at[2], 1)
    share_moments(0)
    for k in range(early, chunks):
        send_own(k)

    left_group = lax.broadcasted_iota(jnp.int32, (channels, channels), 0) // size
    right_group = lax.broadcasted_iota(jnp.int32, (channels, channels), 1) // size
    ones[...] = jnp.where(left_group == right_group, 1.0, 0.0).astype(jnp.bfloat16)
    maxima[...] = jnp.full_like(maxima, -1e30)
    total[...] = jnp.zeros_like(total)
    acc[...] = jnp.zeros_like(acc)

    pltpu.make_async_copy(vector, vector, vector_sem).wait()
    pltpu.make_async_copy(square, square, weight_sem.at[0]).wait()
    with jax.named_scope("fold"):
        wv[...] = jnp.dot(wv[...], wo[...], preferred_element_type=jnp.float32).astype(jnp.bfloat16)
    def relay(s):
        d = s // chunks + 1
        k = s % chunks
        for way, zb in ((0, z - d), (1, z + d)):
            @pl.when(both(no(idle), both(zb >= 0, zb < deep)))
            def _(way=way, zb=zb):
                arrival(zb, k, c).wait_recv()

                @pl.when(open_way(way))
                def _():
                    piece(way, zb, k).start()

                piece(2, zb, k).start()

    with jax.named_scope("early"):
        for s in range(early):
            relay(s)
            if relief and s == 0:
                @pl.when(double)
                def _():
                    forward_detours([(GROUP - 2, k) for k in range(direct, chunks)])

        if relief:
            @pl.when(double)
            def _():
                forward_detours(far[: len(far) // 2])

    with jax.named_scope("stat0"):
        centre, scale = gather_moments(0)
    gain = scale * attn_gain[...]

    def project(positions, first):
        band = slice(first, first + rows)
        normed = ((positions - centre) * gain + attn_shift[...]).astype(jnp.bfloat16)
        query = jnp.dot(normed, wq[...], preferred_element_type=jnp.float32).astype(jnp.bfloat16)
        folded = lax.dot_general(query, wk[...], NT, preferred_element_type=jnp.float32) * (
            LOG2E / math.sqrt(channels)
        )
        queries[band] = (folded * gain).astype(jnp.bfloat16)
        constant = jnp.sum(folded * (attn_shift[...] - centre * gain), axis=1, keepdims=True)
        bias[band] = jnp.broadcast_to(constant, (rows, 128))

    with jax.named_scope("qproj"):
        project(own_rows().astype(jnp.float32), 0)
    if relief:
        @pl.when(double)
        def _():
            with jax.named_scope("second"):
                forward_detours(far[len(far) // 2 :])
                for s in range(early, chunks):
                    relay(s)
                project(kv[z + outward, :, c].reshape(rows, channels).astype(jnp.float32), rows)

    def attend(zb, h, first, count):
        keys = UNIT * cores * chunk
        band = slice(first, first + count)
        block = kv[zb, pl.ds(UNIT * h, UNIT)].reshape(keys, channels)
        scores = lax.dot_general(queries[band], block, NT, preferred_element_type=jnp.float32)
        scores = scores + jnp.tile(bias[band], (1, keys // 128))
        newest = jnp.maximum(maxima[band], jnp.max(scores, axis=1, keepdims=True))
        fade = jnp.exp2(maxima[band] - newest)
        maxima[band] = newest
        expo = jnp.exp2(scores - jnp.tile(newest, (1, keys // 128)))
        summed = total[band] * fade
        for j in range(keys // 128):
            summed = summed + expo[:, j * 128 : (j + 1) * 128]
        total[band] = summed
        product = jnp.dot(expo.astype(jnp.bfloat16), block, preferred_element_type=jnp.float32)
        acc[band] = acc[band] * jnp.tile(fade, (1, channels // 128)) + product

    def settle(zb, h):
        with jax.named_scope("wait"):
            for k in range(UNIT):
                arrival(zb, UNIT * h + k, 1 - c).wait_recv()

    def reach(u):
        needed = (u // units - 1) * chunks + UNIT * (u % units + 1) - 1
        return jnp.minimum(jnp.maximum(u + early, needed), (deep - 1) * chunks - 1)

    def postponed(q, start, span, width):
        inside = both(late, both(q >= start, q < start + span + width))
        moved = jnp.where(q < start + span, q + width, q - span)
        return jnp.where(inside, moved, q)

    done = early + (chunks - early) * double.astype(jnp.int32)

    @pl.loop(0, deep * units)
    def _(u):
        with jax.named_scope("relay"):
            @pl.loop(jnp.maximum(reach(u - 1) + 1, done), jnp.maximum(reach(u) + 1, done))
            def _(q):
                relay(postponed(q, chunks - DETOUR, chunks, DETOUR))

        v = postponed(u, 2 * units - 1, units, 1)
        d = v // units
        h = v % units
        final = both(double, u == (deep - 1) * units - 1)

        @pl.loop(0, 2)
        def _(side):
            zb = z + d * (2 * side - 1)
            inside = both(no(idle), both(zb >= 0, zb < deep))

            @pl.when(both(both(inside, no(final)), jnp.logical_or(side == 0, d > 0)))
            def _():
                settle(zb, h)
                with jax.named_scope("attend"):
                    if relief:
                        @pl.when(double)
                        def _():
                            attend(zb, h, 0, 2 * rows)

                    @pl.when(no(double))
                    def _():
                        attend(zb, h, 0, rows)

    def finish(first):
        band = slice(first, first + rows)
        denominator = jnp.sum(total[band], axis=1, keepdims=True)
        average = (acc[band] / denominator - centre) * gain + attn_shift[...]
        return average.astype(jnp.bfloat16)

    def slab(ref, p):
        return ref.at[pl.ds(p * PIECE, PIECE)]

    def answer_direct(p):
        return hop(
            slab(outgoing, p), slab(answer, p), send_sem.at[3], answer_recv, chief,
            r + 2 * outward,
        )

    def answer_in(p, slot):
        return hop(
            slab(outgoing, p), relayed.at[slot], send_sem.at[3], relayed_recv.at[slot],
            chief - GROUP + 1 + routes[p], r,
        )

    def answer_out(p, slot):
        return hop(
            relayed.at[slot], slab(answer, p), send_sem.at[3], answer_recv, chief,
            r + 2 * outward,
        )

    def leg(route):
        return enumerate(p for p in range(pieces) if routes[p] == route)

    if relief:
        @pl.when(double)
        def _():
            remote = (deep - 1) * lower.astype(jnp.int32)
            settle(remote, units - 1)
            with jax.named_scope("answer"):
                attend(remote, units - 1, rows, rows)
                outgoing[...] = finish(rows)
                for slot in range(slots):
                    for route in (GROUP - 3, GROUP - 2):
                        for other, p in leg(route):
                            if other == slot:
                                answer_in(p, slot).start()
                for _, p in leg(GROUP - 1):
                    answer_direct(p).start()
                attend(remote, units - 1, 0, rows)

        @pl.when(idle)
        def _():
            with jax.named_scope("answered"):
                hop(outgoing, answer, send_sem.at[3], answer_recv, chief, r).wait_recv()

    @pl.when(no(idle))
    def _():
        answer[...] = finish(0)

    with jax.named_scope("post"):
        field = (
            own_rows().astype(jnp.float32)
            + jnp.dot(answer[...], wv[...], preferred_element_type=jnp.float32)
        ).astype(jnp.bfloat16)
        hidden[...] = field
        find_moments(1, field.astype(jnp.float32))
        share_moments(1)

    up = pltpu.make_async_remote_copy(
        src_ref=hidden.at[pl.ds(0, wide)],
        dst_ref=halo.at[1],
        send_sem=halo_send.at[1],
        recv_sem=halo_recv.at[1],
        device_id=(img, r - 1),
        device_id_type=MESH,
    )
    down = pltpu.make_async_remote_copy(
        src_ref=hidden.at[pl.ds(rows - wide, wide)],
        dst_ref=halo.at[0],
        send_sem=halo_send.at[0],
        recv_sem=halo_recv.at[0],
        device_id=(img, r + 1),
        device_id_type=MESH,
    )

    @pl.when(r > 0)
    def _():
        up.start()

    @pl.when(r < n - 1)
    def _():
        down.start()

    if relief:
        for route in (GROUP - 3, GROUP - 2):
            @pl.when(both(helper, member == route))
            def _(route=route):
                with jax.named_scope("leg"):
                    for slot, p in leg(route):
                        answer_in(p, slot).wait_recv()
                        answer_out(p, slot).start()
                    hop(relayed, relayed, send_sem.at[3], answer_recv, chief, r).wait_send()

        @pl.when(double)
        def _():
            hop(detour, detour, send_sem.at[way_out], answer_recv, chief, r).wait_send()
            hop(outgoing, outgoing, send_sem.at[3], answer_recv, chief, r).wait_send()

    def sent(way, first, last):
        part = kv.at[pl.ds(first, last - first), :, c]
        hop(part, part, send_sem.at[way], answer_recv, img, partner).wait_send()

    for here in range(deep):
        if here < deep - 1:
            @pl.when(both(z == here, no(both(is_chief, upper))))
            def _(here=here):
                sent(0, 0, here + 1)

        if here > 0:
            @pl.when(both(z == here, no(both(is_chief, lower))))
            def _(here=here):
                sent(1, here, deep)

    @pl.when(no(idle))
    def _():
        sent(2, 0, deep)

    taps_in.wait()
    with jax.named_scope("stat1"):
        centre, scale = gather_moments(1)
    gain = scale * conv_gain[...]

    def activate(values):
        v = (values.astype(jnp.float32) - centre) * gain + conv_shift[...]
        return (v / (1.0 + jnp.exp(-v))).astype(jnp.bfloat16)

    def place(line, values):
        for dy in range(3):
            y = line + 1 - dy
            if 0 <= y < lines:
                stacked[y * wide : (y + 1) * wide, dy * channels : (dy + 1) * channels] = values

    with jax.named_scope("act"):
      for line in range(lines):
        place(line, activate(hidden[line * wide : (line + 1) * wide]))

    @pl.when(r > 0)
    def _():
        up.wait_send()
        down.wait_recv()
        place(-1, activate(halo[0]))

    @pl.when(r == 0)
    def _():
        place(-1, jnp.zeros((wide, channels), jnp.bfloat16))

    @pl.when(r < n - 1)
    def _():
        down.wait_send()
        up.wait_recv()
        place(lines, activate(halo[1]))

    @pl.when(r == n - 1)
    def _():
        place(lines, jnp.zeros((wide, channels), jnp.bfloat16))

    half = 256
    column = lax.broadcasted_iota(jnp.int32, (rows, half), 0) % wide
    with jax.named_scope("conv"):
      for start in range(0, channels, half):
        cut = slice(start, start + half)

        def taps(dx):
            return jnp.dot(stacked[...], wc[:, dx, :, cut].reshape(3 * channels, half), preferred_element_type=jnp.float32)

        convolved = taps(1)
        convolved = convolved + jnp.where(column > 0, pltpu.roll(taps(0), 1, 0), 0.0)
        convolved = convolved + jnp.where(
            column < wide - 1, pltpu.roll(taps(2), rows - 1, 0), 0.0
        )
        encoded = hidden[:, cut].astype(jnp.float32) + (convolved + conv_bias[:, cut])
        out[:, cut] = encoded.astype(jnp.bfloat16)


def local(n, relief, latent, attn_gain, attn_shift, w_query, w_key, w_value, w_out,
          conv_gain, conv_shift, w_conv, conv_bias):
    height, wide, channels = latent.shape
    rows = height * wide
    chunks = rows // CHUNK
    anywhere = pl.BlockSpec(memory_space=pl.ANY)
    bf16, f32 = jnp.bfloat16, jnp.float32
    dma = pltpu.SemaphoreType.DMA
    encoded = pl.pallas_call(
        functools.partial(kernel, n, relief, wide),
        out_shape=pltpu.VMEM((rows, channels), bf16),
        in_specs=[anywhere] * 11,
        out_specs=pl.BlockSpec(memory_space=pltpu.VMEM),
        scratch_shapes=[
            pltpu.VMEM((5, 1, channels), f32),
            pltpu.VMEM((n // 2, chunks, 2, CHUNK, channels), bf16),
            pltpu.VMEM((4, channels, channels), bf16),
            pltpu.VMEM((3, 3, channels, channels), bf16),
            pltpu.VMEM((channels, channels), bf16),
            pltpu.VMEM((2, n, 2, channels), f32),
            pltpu.VMEM((2 * rows, channels), bf16),
            *[pltpu.VMEM((2 * rows, 128), f32)] * 3,
            pltpu.VMEM((2 * rows, channels), f32),
            pltpu.VMEM((rows, channels), bf16),
            pltpu.VMEM((2, wide, channels), bf16),
            pltpu.VMEM((rows, 3 * channels), bf16),
            dma,
            dma((2,)),
            dma((4,)),
            dma((n // 2, chunks, 2)),
            dma((2,)),
            dma((2,)),
            dma((2,)),
            dma((2,)),
            dma,
            pltpu.SemaphoreType.REGULAR((3,)),
            pltpu.VMEM((GROUP - 1, DETOUR, CHUNK, channels), bf16),
            dma((GROUP - 1, DETOUR)),
            pltpu.VMEM((rows, channels), bf16),
            pltpu.VMEM((rows, channels), bf16),
            dma,
            pltpu.VMEM((rows // PIECE // 4, PIECE, channels), bf16),
            dma((rows // PIECE // 4,)),
        ],
        compiler_params=pltpu.CompilerParams(
            collective_id=0, has_side_effects=True, vmem_limit_bytes=56 * 1024 * 1024
        ),
    )(
        latent.reshape(chunks, CHUNK, channels), w_query, w_key, w_value, w_out, w_conv,
        *(v.reshape(1, channels) for v in (attn_gain, attn_shift, conv_gain, conv_shift, conv_bias)),
    )
    return encoded.reshape(height, wide, channels)


def solution(mesh):
    in_specs = (P(("img", "row"), None, None), P(), P(), P(), P(), P(), P(), P(), P(), P(), P())
    out_specs = P(("img", "row"), None, None)
    images, n = mesh.shape["img"], mesh.shape["row"]
    relief = images % GROUP == 0 and n // 2 >= GROUP
    body = functools.partial(local, n, relief)
    return jax.shard_map(body, mesh=mesh, in_specs=in_specs, out_specs=out_specs, check_vma=False)
```

```python
import functools
import math

import jax
import jax.numpy as jnp
from jax import lax
from jax.experimental import pallas as pl
from jax.experimental.pallas import tpu as pltpu
from jax.sharding import PartitionSpec as P

GROUPS = 32
EPS = 1e-06
CHUNK = 128
UNIT = 2
GROUP = 4
CHIEF = 1
NEAR = (0, 3)
FAR = 2
DETOUR = 2
BRIDGE = 1
PIECE = 64
MESH = pl.DeviceIdType.MESH
LOG2E = math.log2(math.e)
NT = (((1,), (1,)), ((), ()))


def spread_groups(row, ones):
    high = row.astype(jnp.bfloat16).astype(jnp.float32)
    rest = row - high
    mid = rest.astype(jnp.bfloat16).astype(jnp.float32)
    low = rest - mid
    index = lax.broadcasted_iota(jnp.int32, (16, row.shape[1]), 0)
    parts = jnp.where(index == 0, high, jnp.where(index == 1, mid, jnp.where(index == 2, low, 0.0)))
    sums = jnp.dot(parts.astype(jnp.bfloat16), ones, preferred_element_type=jnp.float32)
    return jnp.sum(sums, axis=0, keepdims=True)


def kernel(
    n, relief, wide,
    latent, w_query, w_key, w_value, w_out, w_conv,
    gain_in, shift_in, conv_gain_in, conv_shift_in, bias_in,
    out,
    vector, kv, square, wc, ones, moments, queries, bias, maxima, total, acc, hidden, halo, stacked,
    load_sem, weight_sem, send_sem, recv_sem, stat_send, stat_recv, halo_send, halo_recv,
    vector_sem, present,
    carried, carried_recv, detour, detour_recv, outgoing, answer, answer_recv, relayed, relayed_recv,
):
    chunks, cores, chunk, channels = kv.shape[1:]
    rows = chunks * chunk
    deep = n // 2
    lines = rows // wide
    size = channels // GROUPS
    img = lax.axis_index("img")
    r = lax.axis_index("row")
    z = r // 2
    c = r % 2
    partner = r + 1 - 2 * c
    both = jnp.logical_and
    no = jnp.logical_not
    units = chunks // UNIT
    early = chunks // 2

    member = img % GROUP
    chief = img - member + CHIEF
    is_chief = both(relief, member == CHIEF)
    is_member = both(relief, member != CHIEF)
    lower, upper = z == 1, z == deep - 2
    inner = jnp.logical_or(lower, upper)
    outer = jnp.logical_or(z == 0, z == deep - 1)
    double = both(is_chief, inner)
    idle = both(is_chief, outer)
    helper = both(is_member, inner)
    late = both(is_member, outer)
    bridge = relief and deep == GROUP
    porter = jnp.where(c == 0, NEAR[1], FAR)
    carries = both(both(bridge, helper), member == porter)
    outward = 1 - 2 * lower.astype(jnp.int32)
    inward = 1 - 2 * (z > 0).astype(jnp.int32)
    way_out = lower.astype(jnp.int32)
    direct = chunks - DETOUR
    pieces = rows // PIECE
    routes = [(NEAR[0], NEAR[1], CHIEF, CHIEF, NEAR[0], CHIEF, CHIEF, CHIEF)[p % 8] for p in range(pieces)]

    load = pltpu.make_async_copy(latent, kv.at[z, :, c], load_sem)
    load.start()

    barrier = pltpu.get_barrier_semaphore()

    def neighbours(act):
        @pl.when(z < deep - 1)
        def _():
            act(r + 2)

        @pl.when(z > 0)
        def _():
            act(r - 2)

        act(partner)

    def signal(semaphore, target, image=img):
        pl.semaphore_signal(semaphore, inc=1, device_id=(image, target), device_id_type=MESH)

    neighbours(functools.partial(signal, barrier))
    expected = 1 + (z > 0).astype(jnp.int32) + (z < deep - 1).astype(jnp.int32)
    if relief:
        for i in (*NEAR, FAR):
            @pl.when(double)
            def _(i=i):
                signal(barrier, r, chief - CHIEF + i)

        @pl.when(carries)
        def _():
            signal(barrier, r, chief)

        expected = expected + helper.astype(jnp.int32) + both(bridge, double).astype(jnp.int32)
    vectors = [
        pltpu.make_async_copy(source, vector.at[i], vector_sem)
        for i, source in enumerate((gain_in, shift_in, conv_gain_in, conv_shift_in, bias_in))
    ]
    attn_gain, attn_shift, conv_gain, conv_shift, conv_bias = (vector.at[i] for i in range(5))
    wq, wk, wv, wo = (square.at[i] for i in range(4))
    weights = [
        pltpu.make_async_copy(source, square.at[i], weight_sem.at[0])
        for i, source in enumerate((w_query, w_key, w_value, w_out))
    ]
    taps_in = pltpu.make_async_copy(w_conv, wc, weight_sem.at[1])

    def piece(way, zb, k):
        target = (r + 2, r - 2, partner)[way]
        return pltpu.make_async_remote_copy(
            src_ref=kv.at[zb, k, c],
            dst_ref=kv.at[zb, k, c],
            send_sem=send_sem.at[way],
            recv_sem=recv_sem.at[zb, k, c],
            device_id=(img, target),
            device_id_type=MESH,
        )

    def arrival(zb, k, core):
        return pltpu.make_async_remote_copy(
            src_ref=kv.at[zb, k, core],
            dst_ref=kv.at[zb, k, core],
            send_sem=send_sem.at[0],
            recv_sem=recv_sem.at[zb, k, core],
            device_id=(img, partner),
            device_id_type=MESH,
        )

    def stat_copy(which, j):
        return pltpu.make_async_remote_copy(
            src_ref=moments.at[which, r],
            dst_ref=moments.at[which, r],
            send_sem=stat_send.at[which],
            recv_sem=stat_recv.at[which],
            device_id=(img, lax.rem(r + j, n)),
            device_id_type=MESH,
        )

    def stat_all(which):
        return pltpu.make_async_remote_copy(
            src_ref=moments.at[which, pl.ds(0, n - 1)],
            dst_ref=moments.at[which, pl.ds(0, n - 1)],
            send_sem=stat_send.at[which],
            recv_sem=stat_recv.at[which],
            device_id=(img, partner),
            device_id_type=MESH,
        )

    def own_rows():
        return kv[z, :, c].reshape(rows, channels)

    def hop(source, target, send, recv, image, row):
        return pltpu.make_async_remote_copy(
            src_ref=source,
            dst_ref=target,
            send_sem=send,
            recv_sem=recv,
            device_id=(image, row),
            device_id_type=MESH,
        )

    def detour_in(i, k):
        return hop(
            kv.at[z, k, c], detour.at[i, k - direct], send_sem.at[way_out],
            detour_recv.at[i, k - direct], chief, r,
        )

    def detour_out(i, k):
        return hop(
            detour.at[i, k - direct], kv.at[z, k, c], send_sem.at[way_out],
            recv_sem.at[z, k, c], chief - CHIEF + i, r + 2 * outward,
        )

    def forward_detours(which):
        for i, k in which:
            detour_in(i, k).wait_recv()
            detour_out(i, k).start()

    later = [(i, k) for k in range(direct, chunks) for i in (NEAR[1], FAR)]

    crossing = range(chunks - BRIDGE, chunks)

    def bridge_in(j):
        return hop(
            kv.at[z, crossing[j], c], carried.at[j], send_sem.at[1 - way_out],
            carried_recv.at[j], chief - CHIEF + porter, r,
        )

    def bridge_out(j):
        return hop(
            carried.at[j], kv.at[z, crossing[j], c], send_sem.at[4],
            recv_sem.at[z, crossing[j], c], chief, r - 2 * outward,
        )

    def open_way(way, k=0):
        edge, gate = (z < deep - 1, upper) if way == 0 else (z > 0, lower)
        shut = jnp.logical_or(is_chief, both(is_member, k >= direct))
        return both(edge, no(both(gate, shut)))

    def send_own(k):
        for way in range(2):
            bridged = both(both(bridge and k in crossing, double), way != way_out)

            @pl.when(both(open_way(way, k), no(bridged)))
            def _(way=way):
                piece(way, z, k).start()

        @pl.when(no(idle))
        def _():
            piece(2, z, k).start()

    def send_detours():
        if relief:
            @pl.when(both(bridge, double))
            def _():
                for j in range(BRIDGE):
                    bridge_in(j).start()

            @pl.when(helper)
            def _():
                for k in range(direct, chunks):
                    detour_in(member, k).start()

    def find_moments(which, field):
        mean = jnp.sum(field, axis=0, keepdims=True) * (1.0 / rows)
        offset = field - mean
        square = jnp.sum(offset * offset, axis=0, keepdims=True)
        moments[which, r, 0:1, :] = mean
        moments[which, r, 1:2, :] = square

    def share_moments(which):
        @pl.loop(1, n)
        def _(j):
            stat_copy(which, j).start()

    def gather_moments(which):
        stat_all(which).wait_recv()
        stat_all(which).wait_send()
        every = moments[which]
        means = every[:, 0, :]
        squares = every[:, 1, :]
        centre = spread_groups(jnp.sum(means, axis=0, keepdims=True), ones[...]) * (
            1.0 / (n * size)
        )
        away = means - centre
        whole = jnp.sum(squares + rows * (away * away), axis=0, keepdims=True)
        variance = spread_groups(whole, ones[...]) * (1.0 / (n * size * rows))
        return centre, lax.rsqrt(variance + EPS)

    with jax.named_scope("load"):
        load.wait()
    with jax.named_scope("barrier"):
        pl.semaphore_wait(barrier, expected)

    @pl.when(c == 0)
    def _():
        for k in range(early):
            send_own(k)
        send_detours()

    for copy in vectors + weights + [taps_in]:
        copy.start()
    with jax.named_scope("share0"):
        find_moments(0, own_rows().astype(jnp.float32))

    @pl.when(c == 1)
    def _():
        for k in range(early):
            send_own(k)
        send_detours()

    def chain(way):
        first, last = (z == 0, z == deep - 1) if way == 0 else (z == deep - 1, z == 0)

        @pl.when(jnp.logical_not(first))
        def _():
            pl.semaphore_wait(present.at[way], 1)

        @pl.when(jnp.logical_not(last))
        def _():
            signal(present.at[way], r + 2 - 4 * way)

    with jax.named_scope("present"):
        @pl.when(z < deep // 2)
        def _():
            chain(0)
            chain(1)

        @pl.when(z >= deep // 2)
        def _():
            chain(1)
            chain(0)

        signal(present.at[2], partner)
        pl.semaphore_wait(present.at[2], 1)
    share_moments(0)
    if bridge:
        @pl.when(carries)
        def _():
            for j in range(BRIDGE):
                bridge_in(j).wait_recv()
                bridge_out(j).start()

    for k in range(early, chunks):
        send_own(k)

    left_group = lax.broadcasted_iota(jnp.int32, (channels, channels), 0) // size
    right_group = lax.broadcasted_iota(jnp.int32, (channels, channels), 1) // size
    ones[...] = jnp.where(left_group == right_group, 1.0, 0.0).astype(jnp.bfloat16)
    maxima[...] = jnp.full_like(maxima, -1e30)
    total[...] = jnp.zeros_like(total)
    acc[...] = jnp.zeros_like(acc)

    pltpu.make_async_copy(vector, vector, vector_sem).wait()
    pltpu.make_async_copy(square, square, weight_sem.at[0]).wait()
    with jax.named_scope("fold"):
        wv[...] = jnp.dot(wv[...], wo[...], preferred_element_type=jnp.float32).astype(jnp.bfloat16)
    def relay(s):
        d = s // chunks + 1
        k = s % chunks
        for way, zb in ((0, z - d), (1, z + d)):
            @pl.when(both(no(idle), both(zb >= 0, zb < deep)))
            def _(way=way, zb=zb):
                arrival(zb, k, c).wait_recv()

                @pl.when(open_way(way))
                def _():
                    piece(way, zb, k).start()

                piece(2, zb, k).start()

    with jax.named_scope("early"):
        for s in range(early):
            relay(s)
            if relief and s == 0:
                @pl.when(double)
                def _():
                    forward_detours([(NEAR[0], k) for k in range(direct, chunks)])


    with jax.named_scope("stat0"):
        centre, scale = gather_moments(0)
    gain = scale * attn_gain[...]

    def project(positions, first):
        band = slice(first, first + rows)
        normed = ((positions - centre) * gain + attn_shift[...]).astype(jnp.bfloat16)
        query = jnp.dot(normed, wq[...], preferred_element_type=jnp.float32).astype(jnp.bfloat16)
        folded = lax.dot_general(query, wk[...], NT, preferred_element_type=jnp.float32) * (
            LOG2E / math.sqrt(channels)
        )
        queries[band] = (folded * gain).astype(jnp.bfloat16)
        constant = jnp.sum(folded * (attn_shift[...] - centre * gain), axis=1, keepdims=True)
        bias[band] = jnp.broadcast_to(constant, (rows, 128))

    def attend(zb, h, first, count):
        keys = UNIT * cores * chunk
        band = slice(first, first + count)
        block = kv[zb, pl.ds(UNIT * h, UNIT)].reshape(keys, channels)
        scores = lax.dot_general(queries[band], block, NT, preferred_element_type=jnp.float32)
        scores = scores + jnp.tile(bias[band], (1, keys // 128))
        newest = jnp.maximum(maxima[band], jnp.max(scores, axis=1, keepdims=True))
        fade = jnp.exp2(maxima[band] - newest)
        maxima[band] = newest
        expo = jnp.exp2(scores - jnp.tile(newest, (1, keys // 128)))
        summed = total[band] * fade
        for j in range(keys // 128):
            summed = summed + expo[:, j * 128 : (j + 1) * 128]
        total[band] = summed
        product = jnp.dot(expo.astype(jnp.bfloat16), block, preferred_element_type=jnp.float32)
        acc[band] = acc[band] * jnp.tile(fade, (1, channels // 128)) + product

    def settle(zb, h):
        with jax.named_scope("wait"):
            for k in range(UNIT):
                arrival(zb, UNIT * h + k, 1 - c).wait_recv()

    with jax.named_scope("qproj"):
        project(own_rows().astype(jnp.float32), 0)
    if relief:
        @pl.when(double)
        def _():
            with jax.named_scope("second"):
                settle(z, 0)
                attend(z, 0, 0, rows)
                forward_detours(later[: len(later) // 2])
                for h in range(1, units):
                    settle(z, h)
                    attend(z, h, 0, rows)
                for s in range(early, chunks):
                    relay(s)
                project(kv[z + outward, :, c].reshape(rows, channels).astype(jnp.float32), rows)

    def reach(u):
        needed = (u // units - 1) * chunks + UNIT * (u % units + 1) - 1
        lead = early + double.astype(jnp.int32)
        return jnp.minimum(jnp.maximum(u + lead, needed), (deep - 1) * chunks - 1)

    def postponed(q, start, span, width):
        inside = both(late, both(q >= start, q < start + span + width))
        moved = jnp.where(q < start + span, q + width, q - span)
        return jnp.where(inside, moved, q)

    done = early + (chunks - early) * double.astype(jnp.int32)

    reached = jnp.maximum(z, deep - 1 - z) + 1
    steps = jnp.where(idle, 0, units * reached - double.astype(jnp.int32))

    @pl.loop(0, steps)
    def _(u):
        with jax.named_scope("relay"):
            @pl.loop(jnp.maximum(reach(u - 1) + 1, done), jnp.maximum(reach(u) + 1, done))
            def _(q):
                relay(postponed(q, chunks - DETOUR, chunks + UNIT, DETOUR))

        if relief:
            @pl.when(both(double, u == 1))
            def _():
                forward_detours(later[len(later) // 2 :])

        v = postponed(u, 2 * units - 1, units + 1, 1)
        d = v // units
        h = v % units
        @pl.loop(0, 2)
        def _(side):
            zb = z + d * (2 * side - 1) * (1 - 2 * upper.astype(jnp.int32))
            inside = both(zb >= 0, zb < deep)

            @pl.when(both(inside, jnp.logical_or(side == 0, d > 0)))
            def _():
                @pl.when(no(both(double, d == 0)))
                def _():
                    settle(zb, h)

                with jax.named_scope("attend"):
                    if relief:
                        @pl.when(double)
                        def _():
                            attend(zb, h, rows, rows)

                    @pl.when(no(double))
                    def _():
                        attend(zb, h, 0, rows)

    def finish(first, count):
        band = slice(first, first + count)
        denominator = jnp.sum(total[band], axis=1, keepdims=True)
        average = (acc[band] / denominator - centre) * gain + attn_shift[...]
        return average.astype(jnp.bfloat16)

    def slab(ref, p):
        return ref.at[pl.ds(p * PIECE, PIECE)]

    def answer_direct(p):
        return hop(
            slab(outgoing, p), slab(answer, p), send_sem.at[3], answer_recv, chief,
            r + 2 * outward,
        )

    def answer_in(p, slot):
        return hop(
            slab(outgoing, p), relayed.at[slot], send_sem.at[3], relayed_recv.at[slot],
            chief - CHIEF + routes[p], r,
        )

    def answer_out(p, slot):
        return hop(
            relayed.at[slot], slab(answer, p), send_sem.at[3], answer_recv, chief,
            r + 2 * outward,
        )

    def legs_of(route):
        return [p for p in range(pieces) if routes[p] == route]

    if relief:
        @pl.when(double)
        def _():
            remote = (deep - 1) * lower.astype(jnp.int32)
            settle(remote, units - 1)
            with jax.named_scope("answer"):
                for half in range(2):
                    size = rows // 2
                    attend(remote, units - 1, rows + half * size, size)
                    outgoing[half * size : (half + 1) * size] = finish(rows + half * size, size)
                    for p in range(half * pieces // 2, (half + 1) * pieces // 2):
                        if routes[p] == CHIEF:
                            answer_direct(p).start()
                        else:
                            answer_in(p, legs_of(routes[p]).index(p)).start()

            @pl.loop(units, units * (deep - 1))
            def _(u):
                @pl.loop(0, 2)
                def _(side):
                    zb = z + u // units * (2 * side - 1)

                    @pl.when(both(zb >= 0, zb < deep))
                    def _():
                        attend(zb, u % units, 0, rows)

        for route in NEAR:
            @pl.when(both(helper, member == route))
            def _(route=route):
                with jax.named_scope("leg"):
                    for slot, p in enumerate(legs_of(route)):
                        answer_in(p, slot).wait_recv()
                        answer_out(p, slot).start()

        @pl.when(idle)
        def _():
            with jax.named_scope("answered"):
                hop(outgoing, answer, send_sem.at[3], answer_recv, chief, r).wait_recv()

    @pl.when(no(idle))
    def _():
        answer[...] = finish(0, rows)

    with jax.named_scope("post"):
        field = (
            own_rows().astype(jnp.float32)
            + jnp.dot(answer[...], wv[...], preferred_element_type=jnp.float32)
        ).astype(jnp.bfloat16)
        hidden[...] = field
        find_moments(1, field.astype(jnp.float32))
        share_moments(1)

    up = pltpu.make_async_remote_copy(
        src_ref=hidden.at[pl.ds(0, wide)],
        dst_ref=halo.at[1],
        send_sem=halo_send.at[1],
        recv_sem=halo_recv.at[1],
        device_id=(img, r - 1),
        device_id_type=MESH,
    )
    down = pltpu.make_async_remote_copy(
        src_ref=hidden.at[pl.ds(rows - wide, wide)],
        dst_ref=halo.at[0],
        send_sem=halo_send.at[0],
        recv_sem=halo_recv.at[0],
        device_id=(img, r + 1),
        device_id_type=MESH,
    )

    @pl.when(r > 0)
    def _():
        up.start()

    @pl.when(r < n - 1)
    def _():
        down.start()

    if relief:
        for route in NEAR:
            @pl.when(both(helper, member == route))
            def _(route=route):
                passed = relayed.at[pl.ds(0, len(legs_of(route)))]
                hop(passed, passed, send_sem.at[3], answer_recv, chief, r).wait_send()

        @pl.when(double)
        def _():
            passed = detour.at[pl.ds(0, GROUP - 1)]
            hop(passed, passed, send_sem.at[way_out], answer_recv, chief, r).wait_send()
            hop(outgoing, outgoing, send_sem.at[3], answer_recv, chief, r).wait_send()

        if bridge:
            @pl.when(carries)
            def _():
                hop(carried, carried, send_sem.at[4], answer_recv, chief, r).wait_send()

    def sent(way, first, last):
        part = kv.at[pl.ds(first, last - first), :, c]
        hop(part, part, send_sem.at[way], answer_recv, img, partner).wait_send()

    for here in range(deep):
        if here < deep - 1:
            @pl.when(both(z == here, no(both(is_chief, upper))))
            def _(here=here):
                sent(0, 0, here + 1)

        if here > 0:
            @pl.when(both(z == here, no(both(is_chief, lower))))
            def _(here=here):
                sent(1, here, deep)

    @pl.when(no(idle))
    def _():
        sent(2, 0, deep)

    taps_in.wait()
    with jax.named_scope("stat1"):
        centre, scale = gather_moments(1)
    gain = scale * conv_gain[...]

    def activate(values):
        v = (values.astype(jnp.float32) - centre) * gain + conv_shift[...]
        return (v / (1.0 + jnp.exp(-v))).astype(jnp.bfloat16)

    def place(line, values):
        for dy in range(3):
            y = line + 1 - dy
            if 0 <= y < lines:
                stacked[y * wide : (y + 1) * wide, dy * channels : (dy + 1) * channels] = values

    with jax.named_scope("act"):
      for line in range(lines):
        place(line, activate(hidden[line * wide : (line + 1) * wide]))

    @pl.when(r > 0)
    def _():
        up.wait_send()
        down.wait_recv()
        place(-1, activate(halo[0]))

    @pl.when(r == 0)
    def _():
        place(-1, jnp.zeros((wide, channels), jnp.bfloat16))

    @pl.when(r < n - 1)
    def _():
        down.wait_send()
        up.wait_recv()
        place(lines, activate(halo[1]))

    @pl.when(r == n - 1)
    def _():
        place(lines, jnp.zeros((wide, channels), jnp.bfloat16))

    half = 256
    column = lax.broadcasted_iota(jnp.int32, (rows, half), 0) % wide
    with jax.named_scope("conv"):
      for start in range(0, channels, half):
        cut = slice(start, start + half)

        def taps(dx):
            return jnp.dot(stacked[...], wc[:, dx, :, cut].reshape(3 * channels, half), preferred_element_type=jnp.float32)

        convolved = taps(1)
        convolved = convolved + jnp.where(column > 0, pltpu.roll(taps(0), 1, 0), 0.0)
        convolved = convolved + jnp.where(
            column < wide - 1, pltpu.roll(taps(2), rows - 1, 0), 0.0
        )
        encoded = hidden[:, cut].astype(jnp.float32) + (convolved + conv_bias[:, cut])
        out[:, cut] = encoded.astype(jnp.bfloat16)


def local(n, relief, latent, attn_gain, attn_shift, w_query, w_key, w_value, w_out,
          conv_gain, conv_shift, w_conv, conv_bias):
    height, wide, channels = latent.shape
    rows = height * wide
    chunks = rows // CHUNK
    anywhere = pl.BlockSpec(memory_space=pl.ANY)
    bf16, f32 = jnp.bfloat16, jnp.float32
    dma = pltpu.SemaphoreType.DMA
    encoded = pl.pallas_call(
        functools.partial(kernel, n, relief, wide),
        out_shape=pltpu.VMEM((rows, channels), bf16),
        in_specs=[anywhere] * 11,
        out_specs=pl.BlockSpec(memory_space=pltpu.VMEM),
        scratch_shapes=[
            pltpu.VMEM((5, 1, channels), f32),
            pltpu.VMEM((n // 2, chunks, 2, CHUNK, channels), bf16),
            pltpu.VMEM((4, channels, channels), bf16),
            pltpu.VMEM((3, 3, channels, channels), bf16),
            pltpu.VMEM((channels, channels), bf16),
            pltpu.VMEM((2, n, 2, channels), f32),
            pltpu.VMEM((2 * rows, channels), bf16),
            *[pltpu.VMEM((2 * rows, 128), f32)] * 3,
            pltpu.VMEM((2 * rows, channels), f32),
            pltpu.VMEM((rows, channels), bf16),
            pltpu.VMEM((2, wide, channels), bf16),
            pltpu.VMEM((rows, 3 * channels), bf16),
            dma,
            dma((2,)),
            dma((5,)),
            dma((n // 2, chunks, 2)),
            dma((2,)),
            dma((2,)),
            dma((2,)),
            dma((2,)),
            dma,
            pltpu.SemaphoreType.REGULAR((3,)),
            pltpu.VMEM((BRIDGE, CHUNK, channels), bf16),
            dma((BRIDGE,)),
            pltpu.VMEM((GROUP, DETOUR, CHUNK, channels), bf16),
            dma((GROUP, DETOUR)),
            pltpu.VMEM((rows, channels), bf16),
            pltpu.VMEM((rows, channels), bf16),
            dma,
            pltpu.VMEM((rows // PIECE // 4, PIECE, channels), bf16),
            dma((rows // PIECE // 4,)),
        ],
        compiler_params=pltpu.CompilerParams(
            collective_id=0, has_side_effects=True, vmem_limit_bytes=56 * 1024 * 1024
        ),
    )(
        latent.reshape(chunks, CHUNK, channels), w_query, w_key, w_value, w_out, w_conv,
        *(v.reshape(1, channels) for v in (attn_gain, attn_shift, conv_gain, conv_shift, conv_bias)),
    )
    return encoded.reshape(height, wide, channels)


def solution(mesh):
    in_specs = (P(("img", "row"), None, None), P(), P(), P(), P(), P(), P(), P(), P(), P(), P())
    out_specs = P(("img", "row"), None, None)
    images, n = mesh.shape["img"], mesh.shape["row"]
    relief = images % GROUP == 0 and n // 2 >= GROUP
    body = functools.partial(local, n, relief)
    return jax.shard_map(body, mesh=mesh, in_specs=in_specs, out_specs=out_specs, check_vma=False)
```

```python
import functools
import math

import jax
import jax.numpy as jnp
from jax import lax
from jax.experimental import pallas as pl
from jax.experimental.pallas import tpu as pltpu
from jax.sharding import PartitionSpec as P

GROUPS = 32
EPS = 1e-06
CHUNK = 128
UNIT = 2
GROUP = 4
CHIEF = 1
NEAR = (0, 3)
FAR = 2
DETOUR = 2
BRIDGE = 1
LENT = 1
PIECE = 32
MESH = pl.DeviceIdType.MESH
LOG2E = math.log2(math.e)
NT = (((1,), (1,)), ((), ()))


def spread_groups(row, ones):
    high = row.astype(jnp.bfloat16).astype(jnp.float32)
    rest = row - high
    mid = rest.astype(jnp.bfloat16).astype(jnp.float32)
    low = rest - mid
    lanes = ones.shape[0]
    slices = row.shape[1] // lanes
    depth = -(-3 * slices // 16) * 16
    index = lax.broadcasted_iota(jnp.int32, (depth, lanes), 0)
    parts = jnp.zeros((depth, lanes), jnp.float32)
    for i in range(slices):
        for j, part in enumerate((high, mid, low)):
            piece = part[:, i * lanes : (i + 1) * lanes]
            parts = jnp.where(index == 3 * i + j, piece, parts)
    sums = jnp.dot(parts.astype(jnp.bfloat16), ones, preferred_element_type=jnp.float32)
    return jnp.concatenate(
        [
            jnp.sum(jnp.where(index // 3 == i, sums, 0.0), axis=0, keepdims=True)
            for i in range(slices)
        ],
        axis=1,
    )


def kernel(
    n, relief, wide,
    latent, w_query, w_key, w_value, w_out, w_conv,
    gain_in, shift_in, conv_gain_in, conv_shift_in, bias_in,
    out,
    vector, kv, square, wc, ones, moments, queries, bias, maxima, total, acc, hidden, halo, stacked,
    load_sem, weight_sem, send_sem, recv_sem, stat_send, stat_recv, halo_send, halo_recv,
    vector_sem, present,
    carried, carried_recv, detour, detour_recv, outgoing, answer, answer_recv, relayed, relayed_recv,
):
    chunks, cores, chunk, channels = kv.shape[1:]
    rows = chunks * chunk
    deep = n // 2
    lines = rows // wide
    size = channels // GROUPS
    img = lax.axis_index("img")
    r = lax.axis_index("row")
    z = r // 2
    c = r % 2
    partner = r + 1 - 2 * c
    both = jnp.logical_and
    no = jnp.logical_not
    units = chunks // UNIT
    early = chunks // 2

    member = img % GROUP
    chief = img - member + CHIEF
    is_chief = both(relief, member == CHIEF)
    is_member = both(relief, member != CHIEF)
    lower, upper = z == 1, z == deep - 2
    inner = jnp.logical_or(lower, upper)
    outer = jnp.logical_or(z == 0, z == deep - 1)
    double = both(is_chief, inner)
    idle = both(is_chief, outer)
    helper = both(is_member, inner)
    late = both(is_member, outer)
    bridge = relief and deep == GROUP
    porter = jnp.where(c == 0, NEAR[1], FAR)
    carries = both(both(bridge, helper), member == porter)
    outward = 1 - 2 * lower.astype(jnp.int32)
    inward = 1 - 2 * (z > 0).astype(jnp.int32)
    way_out = lower.astype(jnp.int32)
    direct = chunks - DETOUR
    pieces = rows // PIECE
    routes = [(NEAR[0], NEAR[0], NEAR[1], NEAR[1], CHIEF, CHIEF, CHIEF, CHIEF, NEAR[0], NEAR[0], CHIEF, CHIEF, CHIEF, CHIEF, CHIEF, CHIEF)[p % 16] for p in range(pieces)]

    load = pltpu.make_async_copy(latent, kv.at[z, :, c], load_sem)
    load.start()

    barrier = pltpu.get_barrier_semaphore()

    def neighbours(act):
        @pl.when(z < deep - 1)
        def _():
            act(r + 2)

        @pl.when(z > 0)
        def _():
            act(r - 2)

        act(partner)

    def signal(semaphore, target, image=img):
        pl.semaphore_signal(semaphore, inc=1, device_id=(image, target), device_id_type=MESH)

    neighbours(functools.partial(signal, barrier))
    expected = 1 + (z > 0).astype(jnp.int32) + (z < deep - 1).astype(jnp.int32)
    if relief:
        for i in (*NEAR, FAR):
            @pl.when(double)
            def _(i=i):
                signal(barrier, r, chief - CHIEF + i)

        @pl.when(carries)
        def _():
            signal(barrier, r, chief)

        expected = expected + helper.astype(jnp.int32) + both(bridge, double).astype(jnp.int32)
    vectors = [
        pltpu.make_async_copy(source, vector.at[i], vector_sem)
        for i, source in enumerate((gain_in, shift_in, conv_gain_in, conv_shift_in, bias_in))
    ]
    attn_gain, attn_shift, conv_gain, conv_shift, conv_bias = (vector.at[i] for i in range(5))
    wq, wk, wv, wo = (square.at[i] for i in range(4))
    weights = [
        pltpu.make_async_copy(source, square.at[i], weight_sem.at[0])
        for i, source in enumerate((w_query, w_key, w_value, w_out))
    ]
    taps_in = pltpu.make_async_copy(w_conv, wc, weight_sem.at[1])

    def piece(way, zb, k):
        target = (r + 2, r - 2, partner)[way]
        return pltpu.make_async_remote_copy(
            src_ref=kv.at[zb, k, c],
            dst_ref=kv.at[zb, k, c],
            send_sem=send_sem.at[way],
            recv_sem=recv_sem.at[zb, k, c],
            device_id=(img, target),
            device_id_type=MESH,
        )

    def arrival(zb, k, core):
        return pltpu.make_async_remote_copy(
            src_ref=kv.at[zb, k, core],
            dst_ref=kv.at[zb, k, core],
            send_sem=send_sem.at[0],
            recv_sem=recv_sem.at[zb, k, core],
            device_id=(img, partner),
            device_id_type=MESH,
        )

    def stat_copy(which, j):
        return pltpu.make_async_remote_copy(
            src_ref=moments.at[which, r],
            dst_ref=moments.at[which, r],
            send_sem=stat_send.at[which],
            recv_sem=stat_recv.at[which],
            device_id=(img, lax.rem(r + j, n)),
            device_id_type=MESH,
        )

    def stat_all(which):
        return pltpu.make_async_remote_copy(
            src_ref=moments.at[which, pl.ds(0, n - 1)],
            dst_ref=moments.at[which, pl.ds(0, n - 1)],
            send_sem=stat_send.at[which],
            recv_sem=stat_recv.at[which],
            device_id=(img, partner),
            device_id_type=MESH,
        )

    def lent(way, zb):
        target = (r + 2, r - 2, partner)[way]
        return hop(
            kv.at[zb, LENT, 0], kv.at[zb, LENT, 0], send_sem.at[5 + way],
            recv_sem.at[zb, LENT, 0], img, target,
        )

    def own_rows():
        return kv[z, :, c].reshape(rows, channels)

    def hop(source, target, send, recv, image, row):
        return pltpu.make_async_remote_copy(
            src_ref=source,
            dst_ref=target,
            send_sem=send,
            recv_sem=recv,
            device_id=(image, row),
            device_id_type=MESH,
        )

    def detour_in(i, k):
        return hop(
            kv.at[z, k, c], detour.at[i, k - direct], send_sem.at[way_out],
            detour_recv.at[i, k - direct], chief, r,
        )

    def detour_out(i, k):
        return hop(
            detour.at[i, k - direct], kv.at[z, k, c], send_sem.at[way_out],
            recv_sem.at[z, k, c], chief - CHIEF + i, r + 2 * outward,
        )

    def forward_detours(which):
        for i, k in which:
            detour_in(i, k).wait_recv()
            detour_out(i, k).start()

    later = [(i, k) for k in range(direct, chunks) for i in (NEAR[1], FAR)]

    crossing = range(chunks - BRIDGE, chunks)

    def bridge_in(j):
        return hop(
            kv.at[z, crossing[j], c], carried.at[j], send_sem.at[1 - way_out],
            carried_recv.at[j], chief - CHIEF + porter, r,
        )

    def bridge_out(j):
        return hop(
            carried.at[j], kv.at[z, crossing[j], c], send_sem.at[4],
            recv_sem.at[z, crossing[j], c], chief, r - 2 * outward,
        )

    def open_way(way, k=0):
        edge, gate = (z < deep - 1, upper) if way == 0 else (z > 0, lower)
        shut = jnp.logical_or(is_chief, both(is_member, k >= direct))
        return both(edge, no(both(gate, shut)))

    def send_own(k):
        for way in range(2):
            bridged = both(both(bridge and k in crossing, double), way != way_out)

            mine = both(open_way(way, k), no(bridged))

            @pl.when(both(mine, c == 1) if k == LENT else mine)
            def _(way=way):
                piece(way, z, k).start()

        if k == LENT:
            @pl.when(c == 0)
            def _():
                lent(2, z).start()

        @pl.when(both(no(idle), no(both(c == 0, k == LENT))))
        def _():
            piece(2, z, k).start()

    def send_detours():
        if relief:
            @pl.when(both(bridge, double))
            def _():
                for j in range(BRIDGE):
                    bridge_in(j).start()

            @pl.when(helper)
            def _():
                for k in range(direct, chunks):
                    detour_in(member, k).start()

    def find_moments(which, field):
        mean = jnp.sum(field, axis=0, keepdims=True) * (1.0 / rows)
        offset = field - mean
        square = jnp.sum(offset * offset, axis=0, keepdims=True)
        moments[which, r, 0:1, :] = mean
        moments[which, r, 1:2, :] = square

    def share_moments(which):
        @pl.loop(1, n)
        def _(j):
            stat_copy(which, j).start()

    def gather_moments(which):
        stat_all(which).wait_recv()
        stat_all(which).wait_send()
        every = moments[which]
        means = every[:, 0, :]
        squares = every[:, 1, :]
        centre = spread_groups(jnp.sum(means, axis=0, keepdims=True), ones[...]) * (
            1.0 / (n * size)
        )
        away = means - centre
        whole = jnp.sum(squares + rows * (away * away), axis=0, keepdims=True)
        variance = spread_groups(whole, ones[...]) * (1.0 / (n * size * rows))
        return centre, lax.rsqrt(variance + EPS)

    with jax.named_scope("load"):
        load.wait()
    with jax.named_scope("barrier"):
        pl.semaphore_wait(barrier, expected)

    @pl.when(c == 0)
    def _():
        for k in range(early):
            send_own(k)
        send_detours()

    for copy in vectors + weights + [taps_in]:
        copy.start()
    with jax.named_scope("share0"):
        find_moments(0, own_rows().astype(jnp.float32))

    @pl.when(c == 1)
    def _():
        for k in range(early):
            send_own(k)
        send_detours()

    @pl.when(c == 1)
    def _():
        lent(2, z).wait_recv()
        for way in range(2):
            @pl.when(open_way(way))
            def _(way=way):
                lent(way, z).start()

    def chain(way):
        first, last = (z == 0, z == deep - 1) if way == 0 else (z == deep - 1, z == 0)

        @pl.when(jnp.logical_not(first))
        def _():
            pl.semaphore_wait(present.at[way], 1)

        @pl.when(jnp.logical_not(last))
        def _():
            signal(present.at[way], r + 2 - 4 * way)

    with jax.named_scope("present"):
        @pl.when(z < deep // 2)
        def _():
            chain(0)
            chain(1)

        @pl.when(z >= deep // 2)
        def _():
            chain(1)
            chain(0)

        signal(present.at[2], partner)
        pl.semaphore_wait(present.at[2], 1)
    share_moments(0)
    if bridge:
        @pl.when(carries)
        def _():
            for j in range(BRIDGE):
                bridge_in(j).wait_recv()
                bridge_out(j).start()

    for k in range(early, chunks):
        send_own(k)

    left_group = lax.broadcasted_iota(jnp.int32, ones.shape, 0) // size
    right_group = lax.broadcasted_iota(jnp.int32, ones.shape, 1) // size
    ones[...] = jnp.where(left_group == right_group, 1.0, 0.0).astype(jnp.bfloat16)
    maxima[...] = jnp.full_like(maxima, -1e30)
    total[...] = jnp.zeros_like(total)
    acc[...] = jnp.zeros_like(acc)

    pltpu.make_async_copy(vector, vector, vector_sem).wait()
    pltpu.make_async_copy(square, square, weight_sem.at[0]).wait()
    with jax.named_scope("fold"):
        wv[...] = jnp.dot(wv[...], wo[...], preferred_element_type=jnp.float32).astype(jnp.bfloat16)
    def relay(s):
        d = s // chunks + 1
        k = s % chunks
        for way, zb in ((0, z - d), (1, z + d)):
            inside = both(no(idle), both(zb >= 0, zb < deep))

            @pl.when(both(inside, no(both(c == 0, k == LENT))))
            def _(way=way, zb=zb):
                arrival(zb, k, c).wait_recv()

                @pl.when(open_way(way))
                def _():
                    piece(way, zb, k).start()

                piece(2, zb, k).start()

            @pl.when(both(inside, both(c == 1, k == LENT)))
            def _(way=way, zb=zb):
                lent(way, zb).wait_recv()

                @pl.when(open_way(way))
                def _():
                    lent(way, zb).start()

                lent(2, zb).start()

    with jax.named_scope("early"):
        for s in range(early):
            relay(s)
            if relief and s == 0:
                @pl.when(double)
                def _():
                    forward_detours([(NEAR[0], k) for k in range(direct, chunks)])


    with jax.named_scope("stat0"):
        centre, scale = gather_moments(0)
    gain = scale * attn_gain[...]

    def project(positions, first):
        band = slice(first, first + rows)
        normed = ((positions - centre) * gain + attn_shift[...]).astype(jnp.bfloat16)
        query = jnp.dot(normed, wq[...], preferred_element_type=jnp.float32).astype(jnp.bfloat16)
        folded = lax.dot_general(query, wk[...], NT, preferred_element_type=jnp.float32) * (
            LOG2E / math.sqrt(channels)
        )
        queries[band] = (folded * gain).astype(jnp.bfloat16)
        constant = jnp.sum(folded * (attn_shift[...] - centre * gain), axis=1, keepdims=True)
        bias[band] = jnp.broadcast_to(constant, (rows, 128))

    def attend(zb, h, first, count):
        keys = UNIT * cores * chunk
        band = slice(first, first + count)
        block = kv[zb, pl.ds(UNIT * h, UNIT)].reshape(keys, channels)
        scores = lax.dot_general(queries[band], block, NT, preferred_element_type=jnp.float32)
        scores = scores + jnp.tile(bias[band], (1, keys // 128))
        newest = jnp.maximum(maxima[band], jnp.max(scores, axis=1, keepdims=True))
        fade = jnp.exp2(maxima[band] - newest)
        maxima[band] = newest
        expo = jnp.exp2(scores - jnp.tile(newest, (1, keys // 128)))
        summed = total[band] * fade
        for j in range(keys // 128):
            summed = summed + expo[:, j * 128 : (j + 1) * 128]
        total[band] = summed
        product = jnp.dot(expo.astype(jnp.bfloat16), block, preferred_element_type=jnp.float32)
        acc[band] = acc[band] * jnp.tile(fade, (1, channels // 128)) + product

    def settle(zb, h):
        with jax.named_scope("wait"):
            for i in range(UNIT):
                k = UNIT * h + i

                @pl.when(no(both(c == 1, k == LENT)))
                def _(k=k):
                    arrival(zb, k, 1 - c).wait_recv()

                known = jnp.logical_or(zb == z, both(double, zb == z + outward))

                @pl.when(both(both(c == 0, k == LENT), no(known)))
                def _(k=k):
                    arrival(zb, k, 0).wait_recv()

    with jax.named_scope("qproj"):
        project(own_rows().astype(jnp.float32), 0)
    if relief:
        @pl.when(double)
        def _():
            with jax.named_scope("second"):
                settle(z, 0)
                attend(z, 0, 0, rows)
                forward_detours(later[: len(later) // 2])
                for h in range(1, units):
                    settle(z, h)
                    attend(z, h, 0, rows)
                for s in range(early, chunks):
                    relay(s)
                @pl.when(c == 0)
                def _():
                    arrival(z + outward, LENT, 0).wait_recv()

                project(kv[z + outward, :, c].reshape(rows, channels).astype(jnp.float32), rows)

    def reach(u):
        needed = (u // units - 1) * chunks + UNIT * (u % units + 1) - 1
        soon = both(late, u == 3 * units - 1).astype(jnp.int32)
        needed = needed + UNIT * soon
        lead = early + double.astype(jnp.int32)
        return jnp.minimum(jnp.maximum(u + lead, needed), (deep - 1) * chunks - 1)

    def postponed(q, start, span, width):
        inside = both(late, both(q >= start, q < start + span + width))
        moved = jnp.where(q < start + span, q + width, q - span)
        return jnp.where(inside, moved, q)

    done = early + (chunks - early) * double.astype(jnp.int32)

    reached = jnp.maximum(z, deep - 1 - z) + 1
    steps = jnp.where(idle, 0, units * reached - double.astype(jnp.int32))

    @pl.loop(0, steps)
    def _(u):
        with jax.named_scope("relay"):
            @pl.loop(jnp.maximum(reach(u - 1) + 1, done), jnp.maximum(reach(u) + 1, done))
            def _(q):
                relay(postponed(q, chunks - DETOUR, chunks + UNIT, DETOUR))

        if relief:
            @pl.when(both(double, u == 1))
            def _():
                forward_detours(later[len(later) // 2 :])

        v = postponed(u, 2 * units - 1, units + 1, 1)
        d = v // units
        h = v % units
        @pl.loop(0, 2)
        def _(side):
            zb = z + d * (2 * side - 1) * (1 - 2 * upper.astype(jnp.int32))
            inside = both(zb >= 0, zb < deep)

            @pl.when(both(inside, jnp.logical_or(side == 0, d > 0)))
            def _():
                @pl.when(no(both(double, d == 0)))
                def _():
                    settle(zb, h)

                with jax.named_scope("attend"):
                    if relief:
                        @pl.when(double)
                        def _():
                            attend(zb, h, rows, rows)

                    @pl.when(no(double))
                    def _():
                        attend(zb, h, 0, rows)

    def finish(first, count):
        band = slice(first, first + count)
        denominator = jnp.sum(total[band], axis=1, keepdims=True)
        average = (acc[band] * (1.0 / denominator) - centre) * gain + attn_shift[...]
        return average.astype(jnp.bfloat16)

    def slab(ref, p):
        return ref.at[pl.ds(p * PIECE, PIECE)]

    def answer_direct(p):
        return hop(
            slab(outgoing, p), slab(answer, p), send_sem.at[3], answer_recv, chief,
            r + 2 * outward,
        )

    def answer_in(p, slot):
        return hop(
            slab(outgoing, p), relayed.at[slot], send_sem.at[3], relayed_recv.at[slot],
            chief - CHIEF + routes[p], r,
        )

    def answer_out(p, slot):
        return hop(
            relayed.at[slot], slab(answer, p), send_sem.at[3], answer_recv, chief,
            r + 2 * outward,
        )

    def legs_of(route):
        return [p for p in range(pieces) if routes[p] == route]

    if relief:
        @pl.when(double)
        def _():
            remote = (deep - 1) * lower.astype(jnp.int32)
            settle(remote, units - 1)
            with jax.named_scope("answer"):
                for half in range(2):
                    size = rows // 2
                    attend(remote, units - 1, rows + half * size, size)
                    outgoing[half * size : (half + 1) * size] = finish(rows + half * size, size)
                    for p in range(half * pieces // 2, (half + 1) * pieces // 2):
                        if routes[p] == CHIEF:
                            answer_direct(p).start()
                        else:
                            answer_in(p, legs_of(routes[p]).index(p)).start()

            @pl.loop(units, units * (deep - 1))
            def _(u):
                @pl.loop(0, 2)
                def _(side):
                    zb = z + u // units * (2 * side - 1)

                    @pl.when(both(zb >= 0, zb < deep))
                    def _():
                        attend(zb, u % units, 0, rows)

        for route in NEAR:
            @pl.when(both(helper, member == route))
            def _(route=route):
                with jax.named_scope("leg"):
                    for slot, p in enumerate(legs_of(route)):
                        answer_in(p, slot).wait_recv()
                        answer_out(p, slot).start()

        @pl.when(idle)
        def _():
            with jax.named_scope("answered"):
                hop(outgoing, answer, send_sem.at[3], answer_recv, chief, r).wait_recv()

    @pl.when(no(idle))
    def _():
        answer[...] = finish(0, rows)

    with jax.named_scope("post"):
        field = (
            own_rows().astype(jnp.float32)
            + jnp.dot(answer[...], wv[...], preferred_element_type=jnp.float32)
        ).astype(jnp.bfloat16)
        hidden[...] = field
        find_moments(1, field.astype(jnp.float32))
        share_moments(1)

    up = pltpu.make_async_remote_copy(
        src_ref=hidden.at[pl.ds(0, wide)],
        dst_ref=halo.at[1],
        send_sem=halo_send.at[1],
        recv_sem=halo_recv.at[1],
        device_id=(img, r - 1),
        device_id_type=MESH,
    )
    down = pltpu.make_async_remote_copy(
        src_ref=hidden.at[pl.ds(rows - wide, wide)],
        dst_ref=halo.at[0],
        send_sem=halo_send.at[0],
        recv_sem=halo_recv.at[0],
        device_id=(img, r + 1),
        device_id_type=MESH,
    )

    @pl.when(r > 0)
    def _():
        up.start()

    @pl.when(r < n - 1)
    def _():
        down.start()

    if relief:
        for route in NEAR:
            @pl.when(both(helper, member == route))
            def _(route=route):
                passed = relayed.at[pl.ds(0, len(legs_of(route)))]
                hop(passed, passed, send_sem.at[3], answer_recv, chief, r).wait_send()

        @pl.when(double)
        def _():
            passed = detour.at[pl.ds(0, GROUP - 1)]
            hop(passed, passed, send_sem.at[way_out], answer_recv, chief, r).wait_send()
            hop(outgoing, outgoing, send_sem.at[3], answer_recv, chief, r).wait_send()

        if bridge:
            @pl.when(carries)
            def _():
                hop(carried, carried, send_sem.at[4], answer_recv, chief, r).wait_send()

    def sent(way, first, last):
        blocks = pl.ds(first, last - first)

        def drained(part, semaphore):
            hop(part, part, semaphore, answer_recv, img, partner).wait_send()

        @pl.when(c == 0)
        def _():
            drained(kv.at[blocks, pl.ds(0, chunks - 1), 0], send_sem.at[way])

        @pl.when(c == 1)
        def _():
            drained(kv.at[blocks, :, 1], send_sem.at[way])
            drained(kv.at[blocks, LENT, 0], send_sem.at[5 + way])

    for here in range(deep):
        if here < deep - 1:
            @pl.when(both(z == here, no(both(is_chief, upper))))
            def _(here=here):
                sent(0, 0, here + 1)

        if here > 0:
            @pl.when(both(z == here, no(both(is_chief, lower))))
            def _(here=here):
                sent(1, here, deep)

    @pl.when(both(no(idle), c == 0))
    def _():
        part = kv.at[pl.ds(0, deep), pl.ds(0, chunks - 1), 0]
        hop(part, part, send_sem.at[2], answer_recv, img, partner).wait_send()

    @pl.when(c == 0)
    def _():
        lent(2, z).wait_send()

    @pl.when(both(no(idle), c == 1))
    def _():
        part = kv.at[pl.ds(0, deep), :, 1]
        hop(part, part, send_sem.at[2], answer_recv, img, partner).wait_send()
        part = kv.at[pl.ds(0, deep - 1), LENT, 0]
        hop(part, part, send_sem.at[7], answer_recv, img, partner).wait_send()

    taps_in.wait()
    with jax.named_scope("stat1"):
        centre, scale = gather_moments(1)
    half_gain = 0.5 * scale * conv_gain[...]
    half_shift = 0.5 * conv_shift[...] - centre * half_gain

    def activate(values):
        u = values.astype(jnp.float32) * half_gain + half_shift
        return (u + u * jnp.tanh(u)).astype(jnp.bfloat16)

    def place(line, values):
        for dy in range(3):
            y = line + 1 - dy
            if 0 <= y < lines:
                stacked[y * wide : (y + 1) * wide, dy * channels : (dy + 1) * channels] = values

    with jax.named_scope("act"):
      for line in range(lines):
        place(line, activate(hidden[line * wide : (line + 1) * wide]))

    @pl.when(r > 0)
    def _():
        up.wait_send()
        down.wait_recv()
        place(-1, activate(halo[0]))

    @pl.when(r == 0)
    def _():
        place(-1, jnp.zeros((wide, channels), jnp.bfloat16))

    @pl.when(r < n - 1)
    def _():
        down.wait_send()
        up.wait_recv()
        place(lines, activate(halo[1]))

    @pl.when(r == n - 1)
    def _():
        place(lines, jnp.zeros((wide, channels), jnp.bfloat16))

    half = 256
    column = lax.broadcasted_iota(jnp.int32, (rows, half), 0) % wide
    with jax.named_scope("conv"):
      for start in range(0, channels, half):
        cut = slice(start, start + half)

        def taps(dx):
            return jnp.dot(stacked[...], wc[:, dx, :, cut].reshape(3 * channels, half), preferred_element_type=jnp.float32)

        convolved = taps(1)
        convolved = convolved + jnp.where(column > 0, pltpu.roll(taps(0), 1, 0), 0.0)
        convolved = convolved + jnp.where(
            column < wide - 1, pltpu.roll(taps(2), rows - 1, 0), 0.0
        )
        encoded = hidden[:, cut].astype(jnp.float32) + (convolved + conv_bias[:, cut])
        out[:, cut] = encoded.astype(jnp.bfloat16)


def local(n, relief, latent, attn_gain, attn_shift, w_query, w_key, w_value, w_out,
          conv_gain, conv_shift, w_conv, conv_bias):
    height, wide, channels = latent.shape
    rows = height * wide
    chunks = rows // CHUNK
    anywhere = pl.BlockSpec(memory_space=pl.ANY)
    bf16, f32 = jnp.bfloat16, jnp.float32
    dma = pltpu.SemaphoreType.DMA
    encoded = pl.pallas_call(
        functools.partial(kernel, n, relief, wide),
        out_shape=pltpu.VMEM((rows, channels), bf16),
        in_specs=[anywhere] * 11,
        out_specs=pl.BlockSpec(memory_space=pltpu.VMEM),
        scratch_shapes=[
            pltpu.VMEM((5, 1, channels), f32),
            pltpu.VMEM((n // 2, chunks, 2, CHUNK, channels), bf16),
            pltpu.VMEM((4, channels, channels), bf16),
            pltpu.VMEM((3, 3, channels, channels), bf16),
            pltpu.VMEM((128, 128), bf16),
            pltpu.VMEM((2, n, 2, channels), f32),
            pltpu.VMEM((2 * rows, channels), bf16),
            *[pltpu.VMEM((2 * rows, 128), f32)] * 3,
            pltpu.VMEM((2 * rows, channels), f32),
            pltpu.VMEM((rows, channels), bf16),
            pltpu.VMEM((2, wide, channels), bf16),
            pltpu.VMEM((rows, 3 * channels), bf16),
            dma,
            dma((2,)),
            dma((8,)),
            dma((n // 2, chunks, 2)),
            dma((2,)),
            dma((2,)),
            dma((2,)),
            dma((2,)),
            dma,
            pltpu.SemaphoreType.REGULAR((3,)),
            pltpu.VMEM((BRIDGE, CHUNK, channels), bf16),
            dma((BRIDGE,)),
            pltpu.VMEM((GROUP, DETOUR, CHUNK, channels), bf16),
            dma((GROUP, DETOUR)),
            pltpu.VMEM((rows, channels), bf16),
            pltpu.VMEM((rows, channels), bf16),
            dma,
            pltpu.VMEM((rows // PIECE // 4, PIECE, channels), bf16),
            dma((rows // PIECE // 4,)),
        ],
        compiler_params=pltpu.CompilerParams(
            collective_id=0, has_side_effects=True, vmem_limit_bytes=56 * 1024 * 1024
        ),
    )(
        latent.reshape(chunks, CHUNK, channels), w_query, w_key, w_value, w_out, w_conv,
        *(v.reshape(1, channels) for v in (attn_gain, attn_shift, conv_gain, conv_shift, conv_bias)),
    )
    return encoded.reshape(height, wide, channels)


def solution(mesh):
    in_specs = (P(("img", "row"), None, None), P(), P(), P(), P(), P(), P(), P(), P(), P(), P())
    out_specs = P(("img", "row"), None, None)
    images, n = mesh.shape["img"], mesh.shape["row"]
    relief = images % GROUP == 0 and n // 2 >= GROUP
    body = functools.partial(local, n, relief)
    return jax.shard_map(body, mesh=mesh, in_specs=in_specs, out_specs=out_specs, check_vma=False)
```
